128 devices in a mesh: field: 4 (over x_hi, core), slab: 32 (over x_lo, z, y).
Axes of the slice: x: 4 (x_hi: 2, x_lo: 2; x = x_hi * 2 + x_lo), y: 4, z: 4, core: 2. Of those that a mesh axis runs over, the one named last changes fastest.
Arguments:
- velocity_u: float32 [512, 512, 512], P('field', 'slab'), may hold values from -6 to 6
- velocity_v: float32 [512, 512, 512], P('field', 'slab'), may hold values from -6 to 6
- scalar_theta: float32 [512, 512, 512], P('field', 'slab'), may hold values from -6 to 6
Outputs:
- spectrum: float32 [4, 320, 320, 320], P('field', 'slab')
The draws below stay inside these ranges and needn't reach their ends.
All inputs are finite; a program needn't handle non-finite values.
Results may differ from the reference program's by a relative error of at most 0.00029.
Values sent between devices are 32-bit elements; how exact they have to be, the bound alone decides.
No kernel may reach another device: no remote copies, remote signals or barrier semaphores. Data moves between devices by JAX's collectives and lax.ppermute only.
A program may use at most 128 MiB of HBM per device.

```python
import jax
import jax.numpy as jnp

N = 512
KEEP = 160


def levels(own_key, shape, cuts, smallest, largest):
    factor_of, own = 1.0, jax.random.fold_in(own_key, 6)
    for axis_at, parts in cuts:
        draws = jnp.exp(jax.random.uniform(jax.random.fold_in(own, axis_at), (parts,), jnp.float32, smallest / len(cuts), largest / len(cuts)))
        factor_of = factor_of * jnp.repeat(draws, shape[axis_at] // parts).reshape([-1 if axis == axis_at else 1 for axis in range(len(shape))])
    return factor_of


def gaussian(rng, extent, width, bound, pieces=(), held_as=jnp.bfloat16):
    entries = jax.random.normal(rng, extent, jnp.float32) * width
    if len(pieces) > 0:
        entries = levels(rng, extent, pieces, -0.22, 0.18) * entries
    return jnp.clip(entries, min=-bound, max=bound).astype(held_as)


def setup_inputs(seed: int = 0) -> dict:
    streams_of = jax.random.split(jax.random.key(seed), 4)
    return {
        "velocity_u": gaussian(streams_of[0], (N, N, N), 1.0, 6.0, ((0, 4), (1, 32)), jnp.float32),
        "velocity_v": gaussian(streams_of[1], (N, N, N), 1.0, 6.0, ((0, 4), (1, 32)), jnp.float32),
        "scalar_theta": gaussian(streams_of[2], (N, N, N), 1.0, 6.0, ((0, 4), (1, 32)), jnp.float32),
    }


def transform_one(field):
    scale = 1.0 / (N * jnp.sqrt(jnp.float32(N)))
    index = ((jnp.arange(2 * KEEP) - KEEP) % N).astype(jnp.int32)
    spec = jnp.fft.rfft(field, axis=2)[:, :, :KEEP]
    spec = jnp.fft.fft(spec, axis=0)[index]
    spec = jnp.fft.fft(spec, axis=1)[:, index]
    spec = spec * scale
    result = jnp.concatenate([jnp.real(spec), jnp.imag(spec)], axis=-1).astype(jnp.float32)
    return result.at[KEEP, KEEP, 0].set(0.0)

def reference(velocity_u, velocity_v, scalar_theta):
    outputs = [transform_one(velocity_u * velocity_u), transform_one(velocity_v * velocity_v), transform_one(velocity_u * velocity_v), transform_one(velocity_u * scalar_theta)]
    return jnp.stack(outputs, axis=0)
```

```python
import functools

import jax
import jax.numpy as jnp
import ml_dtypes
import numpy as np
from jax import lax
from jax.experimental import pallas as pl
from jax.experimental.pallas import tpu as pltpu
from jax.sharding import Mesh
from jax.sharding import PartitionSpec as P

N = 512
KEEP = 160
LANES = 128
XB = 128
CHUNKS = 2
YC = 8
DESTS = 16
PAIRS = 5
ROWS = DESTS * PAIRS * YC
VMEM_LIMIT = 50 * 1024 * 1024


def split_table(table):
    high = table.astype(ml_dtypes.bfloat16)
    low = (table - high.astype(np.float64)).astype(ml_dtypes.bfloat16)
    return np.stack([high, low])


def angles(places, waves):
    return (places * waves % N) * (2.0 * np.pi / N)


def depth_table():
    angle = angles(np.arange(N)[:, None], np.arange(KEEP)[None, :])
    re, im = np.cos(angle), -np.sin(angle)
    zeros = np.zeros((N, 64))
    table = np.concatenate([re[:, :128], im[:, :128], re[:, 128:], im[:, 128:], zeros], axis=1)
    return split_table(table / np.sqrt(N))


def first_table():
    half, e, dest, pair = np.meshgrid(np.arange(2), np.arange(2), np.arange(16), np.arange(5), indexing="ij")
    waves = (half * 160 + dest * 10 + 2 * pair + e - KEEP).reshape(2, KEEP)
    angle = angles(np.arange(2 * XB)[None, None, :], waves[:, :, None])
    table = np.stack([np.cos(angle), np.sin(angle)], axis=2).reshape(2, KEEP, 2, 2, XB)
    return split_table(table / np.sqrt(N))


def second_table(chunk):
    source, y = np.meshgrid(np.arange(16), np.arange(YC), indexing="ij")
    places = (source * 16 + chunk * YC + y).reshape(-1)
    waves = np.arange(2 * KEEP) - KEEP
    angle = angles(places[None, :], waves[:, None])
    table = np.stack([np.cos(angle), np.sin(angle)], axis=1)
    return split_table(table / np.sqrt(N))


def halves(value):
    high = value.astype(jnp.bfloat16)
    return high, (value - high.astype(jnp.float32)).astype(jnp.bfloat16)


def dot(a, b):
    return jnp.dot(a, b, preferred_element_type=jnp.float32)


def turn_tail(tail):
    lane = lax.broadcasted_iota(jnp.int32, tail.shape, 1)
    return jnp.where(lane % 64 < 32, pltpu.roll(tail, 96, 1), -pltpu.roll(tail, 32, 1))


def depth_kernel(place_ref, u_ref, v_ref, t_ref, table_ref, own_ref, send_ref):
    core = place_ref[0]
    first = core == 0
    rows = YC * u_ref.shape[0]

    def load(ref):
        return jnp.concatenate([ref[:, y, :] for y in range(YC)], axis=0)

    u, v, t = load(u_ref), load(v_ref), load(t_ref)
    own_square = jnp.where(first, u, v)
    send_square = jnp.where(first, v, u)
    own_other = jnp.where(first, v, t)
    send_other = jnp.where(first, t, v)
    flip = place_ref[1]
    for ref, group, product in (
        (own_ref, 0, own_square * own_square),
        (send_ref, 0, send_square * send_square),
        (own_ref, 1, u * own_other),
        (send_ref, 1, u * send_other),
    ):
        high, low = halves(product)
        out = dot(high, table_ref[0]) + dot(low, table_ref[0]) + dot(high, table_ref[1])
        ref[group ^ flip] = out.reshape(YC, rows // YC, 384)


def depth_stage(place, u, v, t, table, chunk):
    xb = 32
    block = pl.BlockSpec((xb, YC, N), lambda i: (i, chunk, 0))
    out = pl.BlockSpec((2, YC, xb, 384), lambda i: (0, 0, i, 0))
    shape = jax.ShapeDtypeStruct((2, YC, XB, 384), jnp.float32)
    return pl.pallas_call(
        depth_kernel,
        grid=(XB // xb,),
        in_specs=[
            pl.BlockSpec(memory_space=pltpu.SMEM),
            block,
            block,
            block,
            pl.BlockSpec((2, N, 384), lambda i: (0, 0, 0)),
        ],
        out_specs=[out, out],
        out_shape=[shape, shape],
        compiler_params=pltpu.CompilerParams(vmem_limit_bytes=VMEM_LIMIT),
        cost_estimate=pl.CostEstimate(flops=4 * XB * YC * N * 384 * 6, bytes_accessed=12_000_000, transcendentals=0),
        name="depth",
    )(place, u, v, t, table)


def first_kernel(own_ref, recv_ref, table_ref, near_ref, far_ref):
    y = pl.program_id(0)
    values = jnp.concatenate([own_ref[0, 0], recv_ref[0, 0]], axis=0)
    re, im, tail = values[:, :128], values[:, 128:256], values[:, 256:]
    turned = jnp.concatenate([im, -re, turn_tail(tail)], axis=1)
    high, low = halves(jnp.concatenate([values, turned], axis=0))
    out = dot(table_ref[0], high) + dot(table_ref[1], high) + dot(table_ref[0], low)
    count = DESTS * PAIRS
    for b, ref in enumerate((near_ref, far_ref)):
        even = out[b * 160 : b * 160 + count]
        odd = out[b * 160 + count : b * 160 + 2 * count]
        rows = pl.ds(y, count, stride=YC)
        ref[0, rows, :] = even[:, :128]
        ref[1, rows, :] = even[:, 128:256]
        ref[2, rows, :] = odd[:, :128]
        ref[3, rows, :] = odd[:, 128:256]
        ref[4, rows, :] = even[:, 256:] + pltpu.roll(odd[:, 256:], 64, 1)


def first_stage(own, recv, table, group):
    block = pl.BlockSpec((1, 1, XB, 384), lambda y: (group, y, 0, 0))
    out = pl.BlockSpec((5, ROWS, LANES), lambda y: (0, 0, 0))
    shape = jax.ShapeDtypeStruct((5, ROWS, LANES), jnp.float32)
    return pl.pallas_call(
        first_kernel,
        grid=(YC,),
        in_specs=[block, block, pl.BlockSpec((2, 2 * KEEP, 512), lambda y: (0, 0, 0))],
        out_specs=[out, out],
        out_shape=[shape, shape],
        compiler_params=pltpu.CompilerParams(vmem_limit_bytes=VMEM_LIMIT),
        cost_estimate=pl.CostEstimate(flops=YC * 320 * 512 * 384 * 6, bytes_accessed=7_000_000, transcendentals=0),
        name="first",
    )(own, recv, table)


def second_kernel(place_ref, own_ref, other_ref, table_ref, *refs):
    out_ref = refs[-1]
    parts = []
    for ref in (own_ref, other_ref):
        t = [ref[:, i].reshape(DESTS * YC, LANES) for i in range(5)]
        parts += [jnp.concatenate(t, axis=1), jnp.concatenate([t[1], -t[0], t[3], -t[2], turn_tail(t[4])], axis=1)]
    high, low = halves(jnp.concatenate(parts, axis=0))
    out = dot(table_ref[0], high) + dot(table_ref[1], high) + dot(table_ref[0], low)
    tail = out[:, 512:]
    lane = lax.broadcasted_iota(jnp.int32, tail.shape, 1)
    for e in range(2):
        re, im = out[:, 256 * e : 256 * e + 128], out[:, 256 * e + 128 : 256 * e + 256]
        moved = pltpu.roll(im, 32, 1)
        ends = tail if e == 0 else pltpu.roll(tail, 64, 1)
        pieces = [re, jnp.where(lane < 32, ends, moved), jnp.where(lane < 32, moved, ends)[:, :64]]
        for i, piece in enumerate(pieces):
            span = slice(128 * i, min(128 * (i + 1), 320))
            if len(refs) > 1:
                piece = piece + refs[0][e, :, span]
            out_ref[e, :, span] = piece

    @pl.when((place_ref[2] == 1) & (pl.program_id(0) == 0))
    def _():
        row = out_ref[0, KEEP : KEEP + 1, 0:128]
        first = lax.broadcasted_iota(jnp.int32, row.shape, 1) == 0
        out_ref[0, KEEP : KEEP + 1, 0:128] = jnp.where(first, 0.0, row)


def second_stage(place, own, other, table, before):
    block = pl.BlockSpec((DESTS, 5, YC, LANES), lambda k: (0, 0, k, 0))
    out = pl.BlockSpec((2, 2 * KEEP, 2 * KEEP), lambda k: (k, 0, 0))
    extra = [] if before is None else [before]
    return pl.pallas_call(
        second_kernel,
        grid=(PAIRS,),
        in_specs=[
            pl.BlockSpec(memory_space=pltpu.SMEM),
            block,
            block,
            pl.BlockSpec((2, 2 * KEEP, 512), lambda k: (0, 0, 0)),
        ]
        + [out] * len(extra),
        out_specs=out,
        out_shape=jax.ShapeDtypeStruct((2 * PAIRS, 2 * KEEP, 2 * KEEP), jnp.float32),
        input_output_aliases={4: 0} if extra else {},
        compiler_params=pltpu.CompilerParams(vmem_limit_bytes=VMEM_LIMIT),
        cost_estimate=pl.CostEstimate(flops=PAIRS * 320 * 512 * 640 * 6, bytes_accessed=10_000_000, transcendentals=0),
        name="second",
    )(place, own, other, table, *extra)


def ring(value, flip_high, flip_low):
    moves = [(2 * h + l, 2 * (h ^ flip_high) + (l ^ flip_low)) for h in range(2) for l in range(2)]
    return lax.ppermute(value, ("xh", "xl"), moves)


def spread(value):
    value = value.reshape(5, DESTS, ROWS // DESTS, LANES).transpose(1, 0, 2, 3)
    return lax.all_to_all(value, ("z", "y"), split_axis=0, concat_axis=0, tiled=True)


def shards(velocity_u, velocity_v, scalar_theta):
    high, core, low = lax.axis_index("xh"), lax.axis_index("core"), lax.axis_index("xl")
    owns_mean = (low == 1) & (lax.axis_index("z") == 0) & (lax.axis_index("y") == 0)
    place = jnp.stack([core, high, owns_mean.astype(jnp.int32), low]).astype(jnp.int32)

    table = jnp.asarray(first_table())
    table = jnp.where(low == 0, table, table[:, ::-1])
    table = jnp.where(core == 0, table, table[:, :, :, :, ::-1])
    parity = np.arange(2 * KEEP) % 2
    row_parity = np.repeat(np.arange(2), DESTS * PAIRS)
    sign = jnp.where((high == 1) & (row_parity == 1), -1.0, 1.0).astype(jnp.bfloat16)
    first_rows = (table * sign[None, None, :, None, None, None]).reshape(2, 2 * KEEP, 512)

    own_sign = jnp.where((low == 1) & (parity == 1), -1.0, 1.0).astype(jnp.bfloat16)
    other_sign = jnp.where((low == 0) & (parity == 1), -1.0, 1.0).astype(jnp.bfloat16)
    signs = jnp.stack([own_sign, other_sign], axis=1)[None, :, :, None, None]

    depth_columns = jnp.asarray(depth_table())
    result = None
    for chunk in range(CHUNKS):
        own, send = depth_stage(place, velocity_u, velocity_v, scalar_theta, depth_columns, chunk)
        recv = lax.ppermute(send, "core", [(0, 1), (1, 0)])
        mine, across = first_stage(own, recv, first_rows, 0)
        far, diagonal = first_stage(own, recv, first_rows, 1)
        across = ring(across, 0, 1)
        diagonal = ring(diagonal, 1, 1)
        far = ring(far, 1, 0)
        other = spread(across + diagonal)
        mine = spread(mine + far)
        rows = (jnp.asarray(second_table(chunk))[:, :, None] * signs).reshape(2, 2 * KEEP, 512)
        result = second_stage(place, mine, other, rows, result)
    return result[None]


def solution(mesh):
    fine = Mesh(mesh.devices.reshape(2, 2, 2, 4, 4), ("xh", "core", "xl", "z", "y"))
    spec = P(("xh", "core"), ("xl", "z", "y"), None)
    out_specs = P(("xh", "core"), ("xl", "z", "y"), None, None)
    return jax.shard_map(shards, mesh=fine, in_specs=(spec,) * 3, out_specs=out_specs, check_vma=False)
```

```python
import functools

import jax
import jax.numpy as jnp
import ml_dtypes
import numpy as np
from jax import lax
from jax.experimental import pallas as pl
from jax.experimental.pallas import tpu as pltpu
from jax.sharding import Mesh
from jax.sharding import PartitionSpec as P


N = 512
KEEP = 160
LANES = 128
XB = 128
YC = 8
DESTS = 16
PAIRS = 5
LAST = (3, 2)
VMEM_LIMIT = 50 * 1024 * 1024


def split_table(table):
    high = table.astype(ml_dtypes.bfloat16)
    low = (table - high.astype(np.float64)).astype(ml_dtypes.bfloat16)
    return np.stack([high, low])


def angles(places, waves):
    return (places * waves % N) * (2.0 * np.pi / N)


def depth_table():
    angle = angles(np.arange(N)[:, None], np.arange(KEEP)[None, :])
    re, im = np.cos(angle), -np.sin(angle)
    zeros = np.zeros((N, 64))
    table = np.concatenate([re[:, :128], im[:, :128], re[:, 128:], im[:, 128:], zeros], axis=1)
    return split_table(table / np.sqrt(N))


def first_table():
    half, e, pair, dest = np.meshgrid(np.arange(2), np.arange(2), np.arange(5), np.arange(16), indexing="ij")
    waves = (half * 160 + dest * 10 + 2 * pair + e - KEEP).reshape(2, KEEP)
    angle = angles(np.arange(2 * XB)[None, None, :], waves[:, :, None]).reshape(2, KEEP, 2, XB)
    table = np.stack([np.cos(angle), np.sin(angle)], axis=1).transpose(0, 1, 3, 2, 4)
    return split_table(table / np.sqrt(N))


def second_table(chunk):
    source, y = np.meshgrid(np.arange(16), np.arange(YC), indexing="ij")
    places = (source * 16 + chunk * YC + y).reshape(-1)
    places = places[None, :] + np.array([[0], [256]])
    waves = np.arange(2 * KEEP) - KEEP
    angle = angles(places[:, None, :], waves[None, :, None])
    table = np.concatenate([np.cos(angle), np.sin(angle)], axis=2)
    return split_table(table / np.sqrt(N))


def halves(value):
    high = value.astype(jnp.bfloat16)
    return high, (value - high.astype(jnp.float32)).astype(jnp.bfloat16)


def dot(a, b):
    return jnp.dot(a, b, preferred_element_type=jnp.float32)


def turn_tail(tail):
    lane = lax.broadcasted_iota(jnp.int32, tail.shape, 1)
    return jnp.where(lane % 64 < 32, pltpu.roll(tail, 96, 1), -pltpu.roll(tail, 32, 1))


def params():
    return pltpu.CompilerParams(vmem_limit_bytes=VMEM_LIMIT)


def depth_kernel(group, keeps, place_ref, u_ref, v_ref, t_ref, table_ref, *out_refs):
    first = place_ref[0] == 0
    squares = place_ref[1] == group
    rows = YC * u_ref.shape[0]

    def load(ref):
        return jnp.concatenate([ref[:, y, :] for y in range(YC)], axis=0)

    u, v, t = load(u_ref), load(v_ref), load(t_ref)
    highs, lows = [], []
    for keep in keeps:
        swap = first if keep == 0 else ~first
        a = jnp.where(squares & swap, v, u)
        high, low = halves(a * jnp.where(squares, a, jnp.where(swap, t, v)))
        highs.append(high)
        lows.append(low)
    high, low = jnp.concatenate(highs, axis=0), jnp.concatenate(lows, axis=0)
    out = dot(jnp.concatenate([high, low, high], axis=1), table_ref[...])
    for i, ref in enumerate(out_refs):
        ref[...] = out[i * rows : (i + 1) * rows].reshape(YC, rows // YC, 384)


def depth_stage(place, u, v, t, table, chunk, group, keeps):
    xb = 32
    block = pl.BlockSpec((xb, YC, N), lambda i: (i, chunk, 0))
    out = pl.BlockSpec((YC, xb, 384), lambda i: (0, i, 0))
    shape = jax.ShapeDtypeStruct((YC, XB, 384), jnp.float32)
    return pl.pallas_call(
        functools.partial(depth_kernel, group, keeps),
        grid=(XB // xb,),
        in_specs=[
            pl.BlockSpec(memory_space=pltpu.SMEM),
            block,
            block,
            block,
            pl.BlockSpec((3 * N, 384), lambda i: (0, 0)),
        ],
        out_specs=[out] * len(keeps),
        out_shape=[shape] * len(keeps),
        compiler_params=params(),
        cost_estimate=pl.CostEstimate(
            flops=len(keeps) * XB * YC * N * 384 * 6, bytes_accessed=9_000_000, transcendentals=0
        ),
    )(place, u, v, t, table)


def first_kernel(blocks, splits, place_ref, own_ref, recv_ref, table_ref, *refs):
    core, high_half, low_half = place_ref[0], place_ref[1], place_ref[3]
    step = pl.program_id(0)
    sides = []
    for y in range(2):
        values = jnp.concatenate([own_ref[y], recv_ref[y]], axis=0)
        re, im, tail = values[:, :128], values[:, 128:256], values[:, 256:]
        sides.append(jnp.concatenate([values, jnp.concatenate([im, -re, turn_tail(tail)], axis=1)], axis=0))
    high, low = halves(jnp.concatenate(sides, axis=1))
    data = jnp.concatenate([high, low, high], axis=0)

    def rows_of(half):
        parts = [[table_ref[part, half, cs, core ^ j] for cs in range(2) for j in range(2)] for part in range(2)]
        return jnp.concatenate(parts[0] + parts[0] + parts[1], axis=1)

    out = dot(jnp.concatenate([rows_of(low_half ^ b) for b in blocks], axis=0), data)
    sign = jnp.where(high_half == 1, -1.0, 1.0)
    index = 0
    for b in range(len(blocks)):
        base = 0
        for pairs in splits:
            ref = refs[index]
            index += 1
            stride = 5 * pairs * YC
            for y in range(2):
                for p in range(pairs):
                    row = b * 160 + (base + p) * DESTS
                    even = out[row : row + DESTS, 384 * y : 384 * (y + 1)]
                    odd = out[row + 80 : row + 80 + DESTS, 384 * y : 384 * (y + 1)] * sign
                    tiles = [even[:, :128], even[:, 128:256], odd[:, :128], odd[:, 128:256]]
                    tiles.append(even[:, 256:] + pltpu.roll(odd[:, 256:], 64, 1))
                    for i, tile in enumerate(tiles):
                        start = (i * pairs + p) * YC + 2 * step + y
                        ref[pl.ds(start, DESTS, stride=stride), :] = tile
            base += pairs


def first_stage(place, own, recv, table, blocks, splits):
    block = pl.BlockSpec((2, XB, 384), lambda i: (i, 0, 0))
    sizes = list(splits) * len(blocks)
    outs = [(DESTS * 5 * pairs * YC, LANES) for pairs in sizes]
    results = pl.pallas_call(
        functools.partial(first_kernel, blocks, splits),
        grid=(YC // 2,),
        in_specs=[
            pl.BlockSpec(memory_space=pltpu.SMEM),
            block,
            block,
            pl.BlockSpec(table.shape, lambda i: (0,) * 6),
        ],
        out_specs=[pl.BlockSpec(shape, lambda i: (0, 0)) for shape in outs],
        out_shape=[jax.ShapeDtypeStruct(shape, jnp.float32) for shape in outs],
        compiler_params=params(),
        cost_estimate=pl.CostEstimate(flops=YC * len(blocks) * 160 * 512 * 384 * 6, bytes_accessed=7_000_000, transcendentals=0),
    )(place, own, recv, table)
    return [r.reshape(DESTS, 5, pairs, YC, LANES) for r, pairs in zip(results, sizes)]


def second_kernel(count, fresh, base, place_ref, table_ref, *refs):
    out_ref = refs[-1]
    left, right = [], []
    for side in range(count):
        t = [refs[side][:, i, 0].reshape(DESTS * YC, LANES) for i in range(5)]
        values = jnp.concatenate(t, axis=1)
        turned = jnp.concatenate([t[1], -t[0], t[3], -t[2], turn_tail(t[4])], axis=1)
        high, low = halves(jnp.concatenate([values, turned], axis=0))
        half = place_ref[3] ^ fresh[side]
        left += [table_ref[0, half], table_ref[0, half], table_ref[1, half]]
        right += [high, low, high]
    out = dot(jnp.concatenate(left, axis=1), jnp.concatenate(right, axis=0))
    tail = out[:, 512:]
    lane = lax.broadcasted_iota(jnp.int32, tail.shape, 1)
    for e in range(2):
        re, im = out[:, 256 * e : 256 * e + 128], out[:, 256 * e + 128 : 256 * e + 256]
        moved = pltpu.roll(im, 32, 1)
        ends = tail if e == 0 else pltpu.roll(tail, 64, 1)
        pieces = [re, jnp.where(lane < 32, ends, moved), jnp.where(lane < 32, moved, ends)[:, :64]]
        for i, piece in enumerate(pieces):
            span = slice(128 * i, min(128 * (i + 1), 320))
            if len(refs) > count + 1:
                piece = piece + refs[count][e, :, span]
            out_ref[e, :, span] = piece

    @pl.when((place_ref[2] == 1) & (pl.program_id(0) + base == 0))
    def _():
        row = out_ref[0, KEEP : KEEP + 1, 0:128]
        first = lax.broadcasted_iota(jnp.int32, row.shape, 1) == 0
        out_ref[0, KEEP : KEEP + 1, 0:128] = jnp.where(first, 0.0, row)


def second_stage(place, table, sides, base, before):
    pairs = sides[0][1].shape[2]
    block = pl.BlockSpec((DESTS, 5, 1, YC, LANES), lambda k: (0, 0, k, 0, 0))
    out = pl.BlockSpec((2, 2 * KEEP, 2 * KEEP), lambda k: (k + base, 0, 0))
    extra = [] if before is None else [before]
    count = len(sides)
    return pl.pallas_call(
        functools.partial(second_kernel, count, [s[0] for s in sides], base),
        grid=(pairs,),
        in_specs=[pl.BlockSpec(memory_space=pltpu.SMEM), pl.BlockSpec(table.shape, lambda k: (0,) * 4)]
        + [block] * count
        + [out] * len(extra),
        out_specs=out,
        out_shape=jax.ShapeDtypeStruct((2 * PAIRS, 2 * KEEP, 2 * KEEP), jnp.float32),
        input_output_aliases={2 + count: 0} if extra else {},
        compiler_params=params(),
        cost_estimate=pl.CostEstimate(
            flops=pairs * count * 320 * 256 * 640 * 6, bytes_accessed=3_000_000 * pairs, transcendentals=0
        ),
    )(place, table, *[s[1] for s in sides], *extra)


def ring(value, flip_high, flip_low):
    moves = [(2 * h + l, 2 * (h ^ flip_high) + (l ^ flip_low)) for h in range(2) for l in range(2)]
    return lax.ppermute(value, ("xh", "xl"), moves)


def spread(value):
    return lax.all_to_all(value, ("z", "y"), split_axis=0, concat_axis=0, tiled=True)


def transform(velocity_u, velocity_v, scalar_theta):
    high, core, low = lax.axis_index("xh"), lax.axis_index("core"), lax.axis_index("xl")
    owns_mean = (low == 1) & (lax.axis_index("z") == 0) & (lax.axis_index("y") == 0)
    place = jnp.stack([core, high, owns_mean.astype(jnp.int32), low]).astype(jnp.int32)

    rows = jnp.asarray(first_table())
    split = depth_table()
    columns = jnp.asarray(np.concatenate([split[0], split[0], split[1]], axis=0))
    fields = (velocity_u, velocity_v, scalar_theta)

    def depth(unit, keeps):
        return depth_stage(place, *fields, columns, int(unit[0]), int(unit[1]), keeps)

    def swap(send):
        return lax.ppermute(send, "core", [(0, 1), (1, 0)])

    def first(own, recv, blocks, splits):
        return first_stage(place, own, recv, rows, blocks, splits)

    def near_ring(values):
        return [ring(value, 1, 0) for value in values]

    def far_ring(unit, values):
        return [ring(value, int(unit[1]), 1) for value in values]

    def gather(a, b):
        return spread(jnp.add(a, b))

    def second(chunk, sides, base, result):
        return second_stage(place, jnp.asarray(second_table(chunk)), sides, base, result)

    (send,) = depth("01", (0,))
    recv = swap(send)
    (own,) = depth("01", (1,))
    near = near_ring(first(own, recv, (0,), (PAIRS,)))
    far = far_ring("01", first(own, recv, (1,), (PAIRS,)))

    send, own = depth("00", (0, 1))
    kept, across = first(own, swap(send), (0, 1), (PAIRS,))
    across = far_ring("00", [across])

    send, own = depth("11", (0, 1))
    parts = first(own, swap(send), (0, 1), LAST)
    near_last = near_ring(parts[:2])
    far_last = far_ring("11", parts[2:])

    send, own = depth("10", (0, 1))
    parts = first(own, swap(send), (0, 1), LAST)
    kept_last = parts[:2]
    across_last = far_ring("10", parts[2:])

    mine = gather(kept, near[0])
    other = gather(across[0], far[0])
    mine_last = [gather(a, b) for a, b in zip(kept_last, near_last)]
    other_last = [gather(a, b) for a, b in zip(across_last, far_last)]

    result = second(0, [(0, mine), (1, other)], 0, None)
    result = second(1, [(0, mine_last[0])], 0, result)
    result = second(1, [(0, mine_last[1])], LAST[0], result)
    result = second(1, [(1, other_last[0])], 0, result)
    result = second(1, [(1, other_last[1])], LAST[0], result)
    return result[None]


def solution(mesh):
    fine = Mesh(mesh.devices.reshape(2, 2, 2, 4, 4), ("xh", "core", "xl", "z", "y"))
    spec = P(("xh", "core"), ("xl", "z", "y"), None)
    out_specs = P(("xh", "core"), ("xl", "z", "y"), None, None)
    return jax.shard_map(transform, mesh=fine, in_specs=(spec,) * 3, out_specs=out_specs, check_vma=False)
```

```python
import functools

import jax
import jax.numpy as jnp
import ml_dtypes
import numpy as np
from jax import lax
from jax.experimental import pallas as pl
from jax.experimental.pallas import tpu as pltpu
from jax.sharding import Mesh
from jax.sharding import PartitionSpec as P


N = 512
KEEP = 160
LANES = 128
XB = 128
YC = 8
DESTS = 16
PAIRS = 5
LAST = (3, 2)
VMEM_LIMIT = 50 * 1024 * 1024


def split_table(table):
    high = table.astype(ml_dtypes.bfloat16)
    low = (table - high.astype(np.float64)).astype(ml_dtypes.bfloat16)
    return np.stack([high, low])


def angles(places, waves):
    return (places * waves % N) * (2.0 * np.pi / N)


def depth_table():
    angle = angles(np.arange(N)[:, None], np.arange(KEEP)[None, :])
    re, im = np.cos(angle), -np.sin(angle)
    zeros = np.zeros((N, 64))
    table = np.concatenate([re[:, :128], im[:, :128], re[:, 128:], im[:, 128:], zeros], axis=1)
    return split_table(table / np.sqrt(N))


def first_table():
    half, e, pair, dest = np.meshgrid(np.arange(2), np.arange(2), np.arange(5), np.arange(16), indexing="ij")
    waves = (half * 160 + dest * 10 + 2 * pair + e - KEEP).reshape(2, KEEP)
    angle = angles(np.arange(2 * XB)[None, None, :], waves[:, :, None]).reshape(2, KEEP, 2, XB)
    table = np.stack([np.cos(angle), np.sin(angle)], axis=1).transpose(0, 1, 3, 2, 4)
    return split_table(table / np.sqrt(N))


def second_table(chunk):
    source, y = np.meshgrid(np.arange(16), np.arange(YC), indexing="ij")
    places = (source * 16 + chunk * YC + y).reshape(-1)
    places = places[None, :] + np.array([[0], [256]])
    waves = np.arange(2 * KEEP) - KEEP
    angle = angles(places[:, None, :], waves[None, :, None])
    table = np.concatenate([np.cos(angle), np.sin(angle)], axis=2)
    return split_table(table / np.sqrt(N))


def halves(value):
    high = value.astype(jnp.bfloat16)
    return high, (value - high.astype(jnp.float32)).astype(jnp.bfloat16)


def dot(a, b):
    return jnp.dot(a, b, preferred_element_type=jnp.float32)


def turn_tail(tail):
    lane = lax.broadcasted_iota(jnp.int32, tail.shape, 1)
    return jnp.where(lane % 64 < 32, pltpu.roll(tail, 96, 1), -pltpu.roll(tail, 32, 1))


def params():
    return pltpu.CompilerParams(vmem_limit_bytes=VMEM_LIMIT)


def depth_kernel(group, keeps, place_ref, u_ref, v_ref, t_ref, table_ref, *out_refs):
    first = place_ref[0] == 0
    squares = place_ref[1] == group
    rows = YC * u_ref.shape[0]

    def load(ref):
        return jnp.concatenate([ref[:, y, :] for y in range(YC)], axis=0)

    u, v, t = load(u_ref), load(v_ref), load(t_ref)
    highs, lows = [], []
    for keep in keeps:
        swap = first if keep == 0 else ~first
        a = jnp.where(squares & swap, v, u)
        high, low = halves(a * jnp.where(squares, a, jnp.where(swap, t, v)))
        highs.append(high)
        lows.append(low)
    high, low = jnp.concatenate(highs, axis=0), jnp.concatenate(lows, axis=0)
    out = dot(jnp.concatenate([high, low, high], axis=1), table_ref[...])
    for i, ref in enumerate(out_refs):
        ref[...] = out[i * rows : (i + 1) * rows].reshape(YC, rows // YC, 384)


def depth_stage(place, u, v, t, table, chunk, group, keeps):
    xb = 32
    block = pl.BlockSpec((xb, YC, N), lambda i: (i, chunk, 0))
    out = pl.BlockSpec((YC, xb, 384), lambda i: (0, i, 0))
    shape = jax.ShapeDtypeStruct((YC, XB, 384), jnp.float32)
    return pl.pallas_call(
        functools.partial(depth_kernel, group, keeps),
        grid=(XB // xb,),
        in_specs=[
            pl.BlockSpec(memory_space=pltpu.SMEM),
            block,
            block,
            block,
            pl.BlockSpec((3 * N, 384), lambda i: (0, 0)),
        ],
        out_specs=[out] * len(keeps),
        out_shape=[shape] * len(keeps),
        compiler_params=params(),
        cost_estimate=pl.CostEstimate(
            flops=len(keeps) * XB * YC * N * 384 * 6, bytes_accessed=9_000_000, transcendentals=0
        ),
    )(place, u, v, t, table)


def first_kernel(blocks, splits, place_ref, own_ref, recv_ref, table_ref, *refs):
    core, high_half, low_half = place_ref[0], place_ref[1], place_ref[3]
    step = pl.program_id(0)
    sides = []
    for y in range(2):
        values = jnp.concatenate([own_ref[y], recv_ref[y]], axis=0)
        re, im, tail = values[:, :128], values[:, 128:256], values[:, 256:]
        sides.append(jnp.concatenate([values, jnp.concatenate([im, -re, turn_tail(tail)], axis=1)], axis=0))
    high, low = halves(jnp.concatenate(sides, axis=1))
    data = jnp.concatenate([high, low, high], axis=0)

    def rows_of(half):
        parts = [[table_ref[part, half, cs, core ^ j] for cs in range(2) for j in range(2)] for part in range(2)]
        return jnp.concatenate(parts[0] + parts[0] + parts[1], axis=1)

    out = dot(jnp.concatenate([rows_of(low_half ^ b) for b in blocks], axis=0), data)
    sign = jnp.where(high_half == 1, -1.0, 1.0)
    index = 0
    for b in range(len(blocks)):
        base = 0
        for pairs in splits:
            ref = refs[index]
            index += 1
            stride = 5 * pairs * YC
            for y in range(2):
                for p in range(pairs):
                    row = b * 160 + (base + p) * DESTS
                    even = out[row : row + DESTS, 384 * y : 384 * (y + 1)]
                    odd = out[row + 80 : row + 80 + DESTS, 384 * y : 384 * (y + 1)] * sign
                    tiles = [even[:, :128], even[:, 128:256], odd[:, :128], odd[:, 128:256]]
                    tiles.append(even[:, 256:] + pltpu.roll(odd[:, 256:], 64, 1))
                    for i, tile in enumerate(tiles):
                        start = (i * pairs + p) * YC + 2 * step + y
                        ref[pl.ds(start, DESTS, stride=stride), :] = tile
            base += pairs


def first_stage(place, own, recv, table, blocks, splits):
    block = pl.BlockSpec((2, XB, 384), lambda i: (i, 0, 0))
    sizes = list(splits) * len(blocks)
    outs = [(DESTS * 5 * pairs * YC, LANES) for pairs in sizes]
    results = pl.pallas_call(
        functools.partial(first_kernel, blocks, splits),
        grid=(YC // 2,),
        in_specs=[
            pl.BlockSpec(memory_space=pltpu.SMEM),
            block,
            block,
            pl.BlockSpec(table.shape, lambda i: (0,) * 6),
        ],
        out_specs=[pl.BlockSpec(shape, lambda i: (0, 0)) for shape in outs],
        out_shape=[jax.ShapeDtypeStruct(shape, jnp.float32) for shape in outs],
        compiler_params=params(),
        cost_estimate=pl.CostEstimate(flops=YC * len(blocks) * 160 * 512 * 384 * 6, bytes_accessed=7_000_000, transcendentals=0),
    )(place, own, recv, table)
    return [r.reshape(DESTS, 5, pairs, YC, LANES) for r, pairs in zip(results, sizes)]


def second_kernel(count, fresh, base, place_ref, table_ref, *refs):
    out_ref = refs[-1]
    left, right = [], []
    for side in range(count):
        if len(refs[side].shape) == 5:
            t = [refs[side][:, i, 0].reshape(DESTS * YC, LANES) for i in range(5)]
        else:
            steps = [((place_ref[4] - z) & 3, (place_ref[5] - y) & 3) for z in range(4) for y in range(4)]
            t = [jnp.concatenate([refs[side][e, d, i, 0] for e, d in steps], axis=0) for i in range(5)]
        values = jnp.concatenate(t, axis=1)
        turned = jnp.concatenate([t[1], -t[0], t[3], -t[2], turn_tail(t[4])], axis=1)
        high, low = halves(jnp.concatenate([values, turned], axis=0))
        half = place_ref[3] ^ fresh[side]
        left += [table_ref[0, half], table_ref[0, half], table_ref[1, half]]
        right += [high, low, high]
    out = dot(jnp.concatenate(left, axis=1), jnp.concatenate(right, axis=0))
    tail = out[:, 512:]
    lane = lax.broadcasted_iota(jnp.int32, tail.shape, 1)
    for e in range(2):
        re, im = out[:, 256 * e : 256 * e + 128], out[:, 256 * e + 128 : 256 * e + 256]
        moved = pltpu.roll(im, 32, 1)
        ends = tail if e == 0 else pltpu.roll(tail, 64, 1)
        pieces = [re, jnp.where(lane < 32, ends, moved), jnp.where(lane < 32, moved, ends)[:, :64]]
        for i, piece in enumerate(pieces):
            span = slice(128 * i, min(128 * (i + 1), 320))
            if len(refs) > count + 1:
                piece = piece + refs[count][e, :, span]
            out_ref[e, :, span] = piece

    @pl.when((place_ref[2] == 1) & (pl.program_id(0) + base == 0))
    def _():
        row = out_ref[0, KEEP : KEEP + 1, 0:128]
        first = lax.broadcasted_iota(jnp.int32, row.shape, 1) == 0
        out_ref[0, KEEP : KEEP + 1, 0:128] = jnp.where(first, 0.0, row)


def second_stage(place, table, sides, base, before):
    pairs = sides[0][1].shape[2]
    block = pl.BlockSpec((DESTS, 5, 1, YC, LANES), lambda k: (0, 0, k, 0, 0))
    stepped = pl.BlockSpec((4, 4, 5, 1, YC, LANES), lambda k: (0, 0, 0, k, 0, 0))
    out = pl.BlockSpec((2, 2 * KEEP, 2 * KEEP), lambda k: (k + base, 0, 0))
    extra = [] if before is None else [before]
    count = len(sides)
    return pl.pallas_call(
        functools.partial(second_kernel, count, [s[0] for s in sides], base),
        grid=(pairs,),
        in_specs=[pl.BlockSpec(memory_space=pltpu.SMEM), pl.BlockSpec(table.shape, lambda k: (0,) * 4)]
        + [block if s[1].ndim == 5 else stepped for s in sides]
        + [out] * len(extra),
        out_specs=out,
        out_shape=jax.ShapeDtypeStruct((2 * PAIRS, 2 * KEEP, 2 * KEEP), jnp.float32),
        input_output_aliases={2 + count: 0} if extra else {},
        compiler_params=params(),
        cost_estimate=pl.CostEstimate(
            flops=pairs * count * 320 * 256 * 640 * 6, bytes_accessed=3_000_000 * pairs, transcendentals=0
        ),
    )(place, table, *[s[1] for s in sides], *extra)


def ring(value, flip_high, flip_low):
    moves = [(2 * h + l, 2 * (h ^ flip_high) + (l ^ flip_low)) for h in range(2) for l in range(2)]
    return lax.ppermute(value, ("xh", "xl"), moves)


def spread(value):
    return lax.all_to_all(value, ("z", "y"), split_axis=0, concat_axis=0, tiled=True)


def transform(velocity_u, velocity_v, scalar_theta):
    high, core, low = lax.axis_index("xh"), lax.axis_index("core"), lax.axis_index("xl")
    owns_mean = (low == 1) & (lax.axis_index("z") == 0) & (lax.axis_index("y") == 0)
    z_at, y_at = lax.axis_index("z"), lax.axis_index("y")
    place = jnp.stack([core, high, owns_mean.astype(jnp.int32), low, z_at, y_at]).astype(jnp.int32)

    rows = jnp.asarray(first_table())
    split = depth_table()
    columns = jnp.asarray(np.concatenate([split[0], split[0], split[1]], axis=0))
    fields = (velocity_u, velocity_v, scalar_theta)

    def depth(unit, keeps):
        return depth_stage(place, *fields, columns, int(unit[0]), int(unit[1]), keeps)

    def swap(send):
        return lax.ppermute(send, "core", [(0, 1), (1, 0)])

    def first(own, recv, blocks, splits):
        return first_stage(place, own, recv, rows, blocks, splits)

    def near_ring(values):
        return [ring(value, 1, 0) for value in values]

    def far_ring(unit, values):
        return [ring(value, int(unit[1]), 1) for value in values]

    def gather(a, b):
        return spread(jnp.add(a, b))

    def pick(value, at, axis):
        return lax.dynamic_index_in_dim(value, at & 3, axis, keepdims=False)

    def shift(value, axis, step):
        return lax.ppermute(value, axis, [(i, (i + step) % 4) for i in range(4)])

    def stepwise(a, b):
        a, b = (value.reshape(4, 4, *value.shape[1:]) for value in (a, b))
        blocks = [pick(a, y_at + d, 1) + pick(b, y_at + d, 1) for d in range(4)]
        blocks = [block if d == 0 else shift(block, "y", d) for d, block in enumerate(blocks)]
        groups = [jnp.stack([pick(block, z_at + e, 0) for block in blocks]) for e in range(4)]
        groups = [group if e == 0 else shift(group, "z", e) for e, group in enumerate(groups)]
        return jnp.stack(groups)

    def second(chunk, sides, base, result):
        return second_stage(place, jnp.asarray(second_table(chunk)), sides, base, result)

    (send,) = depth("01", (0,))
    recv = swap(send)
    (own,) = depth("01", (1,))
    near = near_ring(first(own, recv, (0,), (PAIRS,)))
    far = far_ring("01", first(own, recv, (1,), (PAIRS,)))

    send, own = depth("00", (0, 1))
    kept, across = first(own, swap(send), (0, 1), (PAIRS,))
    across = far_ring("00", [across])

    send, own = depth("11", (0, 1))
    parts = first(own, swap(send), (0, 1), LAST)
    near_last = near_ring(parts[:2])
    far_last = far_ring("11", parts[2:])

    send, own = depth("10", (0, 1))
    parts = first(own, swap(send), (0, 1), LAST)
    kept_last = parts[:2]
    across_last = far_ring("10", parts[2:])

    mine = gather(kept, near[0])
    other = stepwise(across[0], far[0])
    mine_last = [gather(a, b) for a, b in zip(kept_last, near_last)]
    other_last = [gather(a, b) for a, b in zip(across_last, far_last)]

    result = second(0, [(0, mine), (1, other)], 0, None)
    result = second(1, [(0, mine_last[0])], 0, result)
    result = second(1, [(0, mine_last[1])], LAST[0], result)
    result = second(1, [(1, other_last[0])], 0, result)
    result = second(1, [(1, other_last[1])], LAST[0], result)
    return result[None]


def solution(mesh):
    fine = Mesh(mesh.devices.reshape(2, 2, 2, 4, 4), ("xh", "core", "xl", "z", "y"))
    spec = P(("xh", "core"), ("xl", "z", "y"), None)
    out_specs = P(("xh", "core"), ("xl", "z", "y"), None, None)
    return jax.shard_map(transform, mesh=fine, in_specs=(spec,) * 3, out_specs=out_specs, check_vma=False)
```

```python
import functools

import jax
import jax.numpy as jnp
import ml_dtypes
import numpy as np
from jax import lax
from jax.experimental import pallas as pl
from jax.experimental.pallas import tpu as pltpu
from jax.sharding import Mesh
from jax.sharding import PartitionSpec as P


N = 512
KEEP = 160
LANES = 128
XB = 128
YC = 8
DESTS = 16
PAIRS = 5
LAST = (3, 2)
VMEM_LIMIT = 50 * 1024 * 1024


def split_table(table):
    high = table.astype(ml_dtypes.bfloat16)
    low = (table - high.astype(np.float64)).astype(ml_dtypes.bfloat16)
    return np.stack([high, low])


def angles(places, waves):
    return (places * waves % N) * (2.0 * np.pi / N)


def depth_table():
    angle = angles(np.arange(N)[:, None], np.arange(KEEP)[None, :])
    re, im = np.cos(angle), -np.sin(angle)
    zeros = np.zeros((N, 64))
    table = np.concatenate([re[:, :128], im[:, :128], re[:, 128:], im[:, 128:], zeros], axis=1)
    return split_table(table / np.sqrt(N))


def first_table():
    half, e, pair, dest = np.meshgrid(np.arange(2), np.arange(2), np.arange(5), np.arange(16), indexing="ij")
    waves = (half * 160 + dest * 10 + 2 * pair + e - KEEP).reshape(2, KEEP)
    angle = angles(np.arange(2 * XB)[None, None, :], waves[:, :, None]).reshape(2, KEEP, 2, XB)
    table = np.stack([np.cos(angle), np.sin(angle)], axis=1).transpose(0, 1, 3, 2, 4)
    return split_table(table / np.sqrt(N))


def second_table(chunk):
    source, y = np.meshgrid(np.arange(16), np.arange(YC), indexing="ij")
    places = (source * 16 + chunk * YC + y).reshape(-1)
    waves = np.arange(2 * KEEP) - KEEP
    angle = angles(places[None, :], waves[:, None])
    table = np.concatenate([np.cos(angle), np.sin(angle)], axis=1)
    return split_table(table / np.sqrt(N))


def halves(value):
    high = value.astype(jnp.bfloat16)
    return high, (value - high.astype(jnp.float32)).astype(jnp.bfloat16)


def dot(a, b):
    return jnp.dot(a, b, preferred_element_type=jnp.float32)


def turn_tail(tail):
    lane = lax.broadcasted_iota(jnp.int32, tail.shape, 1)
    return jnp.where(lane % 64 < 32, pltpu.roll(tail, 96, 1), -pltpu.roll(tail, 32, 1))


def params():
    return pltpu.CompilerParams(vmem_limit_bytes=VMEM_LIMIT)


def depth_kernel(group, keeps, place_ref, u_ref, v_ref, t_ref, table_ref, *out_refs):
    first = place_ref[0] == 0
    squares = place_ref[1] == group
    u, v, t = u_ref[...], v_ref[...], t_ref[...]
    rows = YC * u.shape[0]
    highs, lows = [], []
    for keep in keeps:
        swap = first if keep == 0 else ~first
        a = jnp.where(squares & swap, v, u)
        product = a * jnp.where(squares, a, jnp.where(swap, t, v))
        high, low = halves(jnp.swapaxes(product, 0, 1).reshape(rows, N))
        highs.append(high)
        lows.append(low)
    high, low = jnp.concatenate(highs, axis=0), jnp.concatenate(lows, axis=0)
    table = jnp.concatenate([table_ref[0], table_ref[0], table_ref[1]], axis=0)
    out = dot(jnp.concatenate([high, low, high], axis=1), table)
    for i, ref in enumerate(out_refs):
        ref[...] = out[i * rows : (i + 1) * rows].reshape(YC, rows // YC, 384)


def depth_stage(place, u, v, t, table, chunk, group, keeps):
    xb = 32
    block = pl.BlockSpec((xb, YC, N), lambda i: (i, chunk, 0))
    out = pl.BlockSpec((YC, xb, 384), lambda i: (0, i, 0))
    shape = jax.ShapeDtypeStruct((YC, XB, 384), jnp.float32)
    return pl.pallas_call(
        functools.partial(depth_kernel, group, keeps),
        grid=(XB // xb,),
        in_specs=[
            pl.BlockSpec(memory_space=pltpu.SMEM),
            block,
            block,
            block,
            pl.BlockSpec((2, N, 384), lambda i: (0, 0, 0)),
        ],
        out_specs=[out] * len(keeps),
        out_shape=[shape] * len(keeps),
        compiler_params=params(),
        cost_estimate=pl.CostEstimate(
            flops=len(keeps) * XB * YC * N * 384 * 6, bytes_accessed=9_000_000, transcendentals=0
        ),
    )(place, u, v, t, table)


def first_kernel(blocks, splits, place_ref, own_ref, recv_ref, table_ref, *refs):
    core, high_half, low_half = place_ref[0], place_ref[1], place_ref[3]
    step = pl.program_id(0)
    sides = []
    for y in range(2):
        values = jnp.concatenate([own_ref[y], recv_ref[y]], axis=0)
        re, im, tail = values[:, :128], values[:, 128:256], values[:, 256:]
        sides.append(jnp.concatenate([values, jnp.concatenate([im, -re, turn_tail(tail)], axis=1)], axis=0))
    high, low = halves(jnp.concatenate(sides, axis=1))
    data = jnp.concatenate([high, low, high], axis=0)

    def rows_of(half):
        parts = [[table_ref[part, half, cs, core ^ j] for cs in range(2) for j in range(2)] for part in range(2)]
        return jnp.concatenate(parts[0] + parts[0] + parts[1], axis=1)

    out = dot(jnp.concatenate([rows_of(low_half ^ b) for b in blocks], axis=0), data)
    sign = jnp.where(high_half == 1, -1.0, 1.0)
    index = 0
    for b in range(len(blocks)):
        base = 0
        for pairs in splits[b]:
            ref = refs[index]
            index += 1
            stride = 5 * pairs * YC
            for y in range(2):
                for p in range(pairs):
                    row = b * 160 + (base + p) * DESTS
                    even = out[row : row + DESTS, 384 * y : 384 * (y + 1)]
                    odd = out[row + 80 : row + 80 + DESTS, 384 * y : 384 * (y + 1)] * sign
                    tiles = [even[:, :128], even[:, 128:256], odd[:, :128], odd[:, 128:256]]
                    tiles.append(even[:, 256:] + pltpu.roll(odd[:, 256:], 64, 1))
                    for i, tile in enumerate(tiles):
                        start = (i * pairs + p) * YC + 2 * step + y
                        ref[pl.ds(start, DESTS, stride=stride), :] = tile
            base += pairs


def first_stage(place, own, recv, table, blocks, splits):
    block = pl.BlockSpec((2, XB, 384), lambda i: (i, 0, 0))
    sizes = [pairs for split in splits for pairs in split]
    outs = [(DESTS * 5 * pairs * YC, LANES) for pairs in sizes]
    results = pl.pallas_call(
        functools.partial(first_kernel, blocks, splits),
        grid=(YC // 2,),
        in_specs=[
            pl.BlockSpec(memory_space=pltpu.SMEM),
            block,
            block,
            pl.BlockSpec(table.shape, lambda i: (0,) * 6),
        ],
        out_specs=[pl.BlockSpec(shape, lambda i: (0, 0)) for shape in outs],
        out_shape=[jax.ShapeDtypeStruct(shape, jnp.float32) for shape in outs],
        compiler_params=params(),
        cost_estimate=pl.CostEstimate(flops=YC * len(blocks) * 160 * 512 * 384 * 6, bytes_accessed=7_000_000, transcendentals=0),
    )(place, own, recv, table)
    return [r.reshape(DESTS, 5, pairs, YC, LANES) for r, pairs in zip(results, sizes)]


def second_kernel(count, fresh, base, place_ref, table_ref, *refs):
    out_ref = refs[-1]
    left, right = [], []
    for side in range(count):
        t = [refs[side][:, i, 0].reshape(DESTS * YC, LANES) for i in range(5)]
        values = jnp.concatenate(t, axis=1)
        turned = jnp.concatenate([t[1], -t[0], t[3], -t[2], turn_tail(t[4])], axis=1)
        high, low = halves(jnp.concatenate([values, turned], axis=0))
        odd = lax.broadcasted_iota(jnp.int32, (2 * KEEP, 1), 0) % 2 == 1
        flip = odd & ((place_ref[3] ^ fresh[side]) == 1)
        sign = jnp.where(flip, -1.0, 1.0).astype(jnp.bfloat16)
        left += [table_ref[0] * sign, table_ref[0] * sign, table_ref[1] * sign]
        right += [high, low, high]
    out = dot(jnp.concatenate(left, axis=1), jnp.concatenate(right, axis=0))
    tail = out[:, 512:]
    lane = lax.broadcasted_iota(jnp.int32, tail.shape, 1)
    for e in range(2):
        re, im = out[:, 256 * e : 256 * e + 128], out[:, 256 * e + 128 : 256 * e + 256]
        moved = pltpu.roll(im, 32, 1)
        ends = tail if e == 0 else pltpu.roll(tail, 64, 1)
        pieces = [re, jnp.where(lane < 32, ends, moved), jnp.where(lane < 32, moved, ends)[:, :64]]
        for i, piece in enumerate(pieces):
            span = slice(128 * i, min(128 * (i + 1), 320))
            if len(refs) > count + 1:
                piece = piece + refs[count][e, :, span]
            out_ref[e, :, span] = piece

    @pl.when((place_ref[2] == 1) & (pl.program_id(0) + base == 0))
    def _():
        row = out_ref[0, KEEP : KEEP + 1, 0:128]
        first = lax.broadcasted_iota(jnp.int32, row.shape, 1) == 0
        out_ref[0, KEEP : KEEP + 1, 0:128] = jnp.where(first, 0.0, row)


def second_stage(place, table, sides, base, before):
    pairs = sides[0][1].shape[2]
    block = pl.BlockSpec((DESTS, 5, 1, YC, LANES), lambda k: (0, 0, k, 0, 0))
    out = pl.BlockSpec((2, 2 * KEEP, 2 * KEEP), lambda k: (k + base, 0, 0))
    extra = [] if before is None else [before]
    count = len(sides)
    return pl.pallas_call(
        functools.partial(second_kernel, count, [s[0] for s in sides], base),
        grid=(pairs,),
        in_specs=[pl.BlockSpec(memory_space=pltpu.SMEM), pl.BlockSpec(table.shape, lambda k: (0,) * 3)]
        + [block] * count
        + [out] * len(extra),
        out_specs=out,
        out_shape=jax.ShapeDtypeStruct((2 * PAIRS, 2 * KEEP, 2 * KEEP), jnp.float32),
        input_output_aliases={2 + count: 0} if extra else {},
        compiler_params=params(),
        cost_estimate=pl.CostEstimate(
            flops=pairs * count * 320 * 256 * 640 * 6, bytes_accessed=3_000_000 * pairs, transcendentals=0
        ),
    )(place, table, *[s[1] for s in sides], *extra)


def ring(value, flip_high, flip_low):
    moves = [(2 * h + l, 2 * (h ^ flip_high) + (l ^ flip_low)) for h in range(2) for l in range(2)]
    return lax.ppermute(value, ("xh", "xl"), moves)


def spread(value):
    return lax.all_to_all(value, ("z", "y"), split_axis=0, concat_axis=0, tiled=True)


def transform(velocity_u, velocity_v, scalar_theta):
    high, core, low = lax.axis_index("xh"), lax.axis_index("core"), lax.axis_index("xl")
    owns_mean = (low == 1) & (lax.axis_index("z") == 0) & (lax.axis_index("y") == 0)
    place = jnp.stack([core, high, owns_mean.astype(jnp.int32), low]).astype(jnp.int32)

    rows = jnp.asarray(first_table())
    columns = jnp.asarray(depth_table())
    fields = (velocity_u, velocity_v, scalar_theta)

    def depth(unit, keeps):
        return depth_stage(place, *fields, columns, int(unit[0]), int(unit[1]), keeps)

    def swap(send):
        return lax.ppermute(send, "core", [(0, 1), (1, 0)])

    def first(own, recv, blocks, splits):
        return first_stage(place, own, recv, rows, blocks, splits)

    def near_ring(values):
        return [ring(value, 1, 0) for value in values]

    def far_ring(unit, values):
        return [ring(value, int(unit[1]), 1) for value in values]

    def gather(a, b):
        return spread(jnp.add(a, b))

    def second(chunk, sides, base, result):
        return second_stage(place, jnp.asarray(second_table(chunk)), sides, base, result)

    (send,) = depth("01", (0,))
    recv = swap(send)
    (own,) = depth("01", (1,))
    near = near_ring(first(own, recv, (0,), ((PAIRS,),)))
    far = far_ring("01", first(own, recv, (1,), ((PAIRS,),)))

    send, own = depth("00", (0, 1))
    kept, across = first(own, swap(send), (0, 1), ((PAIRS,), (PAIRS,)))
    across = far_ring("00", [across])

    send, own = depth("11", (0, 1))
    near_last, *far_last = first(own, swap(send), (0, 1), ((PAIRS,), LAST))
    near_last = near_ring([near_last])
    far_last = far_ring("11", far_last)

    send, own = depth("10", (0, 1))
    kept_last, *across_last = first(own, swap(send), (0, 1), ((PAIRS,), LAST))
    across_last = far_ring("10", across_last)

    mine = gather(kept, near[0])
    other = gather(across[0], far[0])
    mine_last = gather(kept_last, near_last[0])
    other_last = [gather(a, b) for a, b in zip(across_last, far_last)]

    result = second(0, [(0, mine), (1, other)], 0, None)
    result = second(1, [(0, mine_last)], 0, result)
    result = second(1, [(1, other_last[0])], 0, result)
    result = second(1, [(1, other_last[1])], LAST[0], result)
    return result[None]


def solution(mesh):
    fine = Mesh(mesh.devices.reshape(2, 2, 2, 4, 4), ("xh", "core", "xl", "z", "y"))
    spec = P(("xh", "core"), ("xl", "z", "y"), None)
    out_specs = P(("xh", "core"), ("xl", "z", "y"), None, None)
    return jax.shard_map(transform, mesh=fine, in_specs=(spec,) * 3, out_specs=out_specs, check_vma=False)
```

```python
import functools

import jax
import jax.numpy as jnp
import ml_dtypes
import numpy as np
from jax import lax
from jax.experimental import pallas as pl
from jax.experimental.pallas import tpu as pltpu
from jax.sharding import Mesh
from jax.sharding import PartitionSpec as P


N = 512
KEEP = 160
LANES = 128
XB = 128
YC = 8
DESTS = 16
PAIRS = 5
EARLY = (3, 2)
VMEM_LIMIT = 24 * 1024 * 1024
DEPTH_LIMIT = 50 * 1024 * 1024


def split_table(table):
    high = table.astype(ml_dtypes.bfloat16)
    low = (table - high.astype(np.float64)).astype(ml_dtypes.bfloat16)
    return np.stack([high, low])


def angles(places, waves):
    return (places * waves % N) * (2.0 * np.pi / N)


def depth_table():
    angle = angles(np.arange(N)[:, None], np.arange(KEEP)[None, :])
    re, im = np.cos(angle), -np.sin(angle)
    zeros = np.zeros((N, 64))
    table = np.concatenate([re[:, :128], im[:, :128], re[:, 128:], im[:, 128:], zeros], axis=1)
    return split_table(table / np.sqrt(N))


def first_table():
    half, e, pair, dest = np.meshgrid(np.arange(2), np.arange(2), np.arange(5), np.arange(16), indexing="ij")
    waves = (half * 160 + dest * 10 + 2 * pair + e - KEEP).reshape(2, KEEP)
    angle = angles(np.arange(2 * XB)[None, None, :], waves[:, :, None]).reshape(2, KEEP, 2, XB)
    table = np.stack([np.cos(angle), np.sin(angle)], axis=1).transpose(0, 1, 3, 2, 4)
    return split_table(table / np.sqrt(N))


def second_table(chunk):
    source, y = np.meshgrid(np.arange(16), np.arange(YC), indexing="ij")
    places = (source * 16 + chunk * YC + y).reshape(-1)
    waves = np.arange(2 * KEEP) - KEEP
    angle = angles(places[None, :], waves[:, None])
    table = np.concatenate([np.cos(angle), np.sin(angle)], axis=1)
    return split_table(table / np.sqrt(N))


def halves(value):
    high = value.astype(jnp.bfloat16)
    return high, (value - high.astype(jnp.float32)).astype(jnp.bfloat16)


def dot(a, b):
    return jnp.dot(a, b, preferred_element_type=jnp.float32)


def turn_tail(tail):
    lane = lax.broadcasted_iota(jnp.int32, tail.shape, 1)
    return jnp.where(lane % 64 < 32, pltpu.roll(tail, 96, 1), -pltpu.roll(tail, 32, 1))


def params(limit=VMEM_LIMIT):
    return pltpu.CompilerParams(vmem_limit_bytes=limit)


def depth_kernel(group, keeps, place_ref, u_ref, v_ref, t_ref, table_ref, *out_refs):
    first = place_ref[0] == 0
    squares = place_ref[1] == group
    u, v, t = u_ref[...], v_ref[...], t_ref[...]
    rows = YC * u.shape[0]
    highs, lows = [], []
    for keep in keeps:
        swap = first if keep == 0 else ~first
        a = jnp.where(squares & swap, v, u)
        product = a * jnp.where(squares, a, jnp.where(swap, t, v))
        high, low = halves(jnp.swapaxes(product, 0, 1).reshape(rows, N))
        highs.append(high)
        lows.append(low)
    high, low = jnp.concatenate(highs, axis=0), jnp.concatenate(lows, axis=0)
    table = jnp.concatenate([table_ref[0], table_ref[0], table_ref[1]], axis=0)
    out = dot(jnp.concatenate([high, low, high], axis=1), table)
    for i, ref in enumerate(out_refs):
        ref[...] = out[i * rows : (i + 1) * rows].reshape(YC, rows // YC, 384)


def depth_stage(place, u, v, t, table, chunk, group, keeps):
    xb = 32
    block = pl.BlockSpec((xb, YC, N), lambda i: (i, chunk, 0))
    out = pl.BlockSpec((YC, xb, 384), lambda i: (0, i, 0))
    shape = jax.ShapeDtypeStruct((YC, XB, 384), jnp.float32)
    return pl.pallas_call(
        functools.partial(depth_kernel, group, keeps),
        grid=(XB // xb,),
        in_specs=[
            pl.BlockSpec(memory_space=pltpu.SMEM),
            block,
            block,
            block,
            pl.BlockSpec((2, N, 384), lambda i: (0, 0, 0)),
        ],
        out_specs=[out] * len(keeps),
        out_shape=[shape] * len(keeps),
        compiler_params=params(DEPTH_LIMIT),
        cost_estimate=pl.CostEstimate(
            flops=len(keeps) * XB * YC * N * 384 * 6, bytes_accessed=9_000_000, transcendentals=0
        ),
    )(place, u, v, t, table)


def first_kernel(blocks, splits, place_ref, own_ref, recv_ref, table_ref, *refs):
    core, high_half, low_half = place_ref[0], place_ref[1], place_ref[3]
    step = pl.program_id(0)
    sides = []
    for y in range(2):
        values = jnp.concatenate([own_ref[y], recv_ref[y]], axis=0)
        re, im, tail = values[:, :128], values[:, 128:256], values[:, 256:]
        sides.append(jnp.concatenate([values, jnp.concatenate([im, -re, turn_tail(tail)], axis=1)], axis=0))
    high, low = halves(jnp.concatenate(sides, axis=1))
    data = jnp.concatenate([high, low, high], axis=0)

    def rows_of(half):
        parts = [[table_ref[part, half, cs, core ^ j] for cs in range(2) for j in range(2)] for part in range(2)]
        return jnp.concatenate(parts[0] + parts[0] + parts[1], axis=1)

    out = dot(jnp.concatenate([rows_of(low_half ^ b) for b in blocks], axis=0), data)
    sign = jnp.where(high_half == 1, -1.0, 1.0)
    index = 0
    for b in range(len(blocks)):
        base = 0
        for pairs in splits[b]:
            ref = refs[index]
            index += 1
            stride = 5 * pairs * YC
            for y in range(2):
                for p in range(pairs):
                    row = b * 160 + (base + p) * DESTS
                    even = out[row : row + DESTS, 384 * y : 384 * (y + 1)]
                    odd = out[row + 80 : row + 80 + DESTS, 384 * y : 384 * (y + 1)] * sign
                    tiles = [even[:, :128], even[:, 128:256], odd[:, :128], odd[:, 128:256]]
                    tiles.append(even[:, 256:] + pltpu.roll(odd[:, 256:], 64, 1))
                    for i, tile in enumerate(tiles):
                        start = (i * pairs + p) * YC + 2 * step + y
                        ref[pl.ds(start, DESTS, stride=stride), :] = tile
            base += pairs


def first_stage(place, own, recv, table, blocks, splits):
    block = pl.BlockSpec((2, XB, 384), lambda i: (i, 0, 0))
    sizes = [pairs for split in splits for pairs in split]
    outs = [(DESTS * 5 * pairs * YC, LANES) for pairs in sizes]
    results = pl.pallas_call(
        functools.partial(first_kernel, blocks, splits),
        grid=(YC // 2,),
        in_specs=[
            pl.BlockSpec(memory_space=pltpu.SMEM),
            block,
            block,
            pl.BlockSpec(table.shape, lambda i: (0,) * 6),
        ],
        out_specs=[pl.BlockSpec(shape, lambda i: (0, 0)) for shape in outs],
        out_shape=[jax.ShapeDtypeStruct(shape, jnp.float32) for shape in outs],
        compiler_params=params(DEPTH_LIMIT),
        cost_estimate=pl.CostEstimate(flops=YC * len(blocks) * 160 * 512 * 384 * 6, bytes_accessed=7_000_000, transcendentals=0),
    )(place, own, recv, table)
    return [r.reshape(DESTS, 5, pairs, YC, LANES) for r, pairs in zip(results, sizes)]


def second_kernel(count, fresh, parts, base, place_ref, table_ref, *refs):
    out_ref = refs[-1]
    left, right = [], []
    at = 0
    for side in range(len(fresh)):
        group = refs[at : at + parts[side]]
        at += parts[side]
        t = [sum(ref[:, i, 0].reshape(DESTS * YC, LANES) for ref in group) for i in range(5)]
        values = jnp.concatenate(t, axis=1)
        turned = jnp.concatenate([t[1], -t[0], t[3], -t[2], turn_tail(t[4])], axis=1)
        high, low = halves(jnp.concatenate([values, turned], axis=0))
        odd = lax.broadcasted_iota(jnp.int32, (2 * KEEP, 1), 0) % 2 == 1
        flip = odd & ((place_ref[3] ^ fresh[side]) == 1)
        sign = jnp.where(flip, -1.0, 1.0).astype(jnp.bfloat16)
        left += [table_ref[0] * sign, table_ref[0] * sign, table_ref[1] * sign]
        right += [high, low, high]
    out = dot(jnp.concatenate(left, axis=1), jnp.concatenate(right, axis=0))
    tail = out[:, 512:]
    lane = lax.broadcasted_iota(jnp.int32, tail.shape, 1)
    for e in range(2):
        re, im = out[:, 256 * e : 256 * e + 128], out[:, 256 * e + 128 : 256 * e + 256]
        moved = pltpu.roll(im, 32, 1)
        ends = tail if e == 0 else pltpu.roll(tail, 64, 1)
        pieces = [re, jnp.where(lane < 32, ends, moved), jnp.where(lane < 32, moved, ends)[:, :64]]
        for i, piece in enumerate(pieces):
            span = slice(128 * i, min(128 * (i + 1), 320))
            if len(refs) > count + 1:
                piece = piece + refs[count][e, :, span]
            out_ref[e, :, span] = piece

    @pl.when((place_ref[2] == 1) & (pl.program_id(0) + base == 0))
    def _():
        row = out_ref[0, KEEP : KEEP + 1, 0:128]
        first = lax.broadcasted_iota(jnp.int32, row.shape, 1) == 0
        out_ref[0, KEEP : KEEP + 1, 0:128] = jnp.where(first, 0.0, row)


def second_stage(place, table, sides, base, before):
    values = [value for side in sides for value in side[1:]]
    pairs = values[0].shape[2]
    block = pl.BlockSpec((DESTS, 5, 1, YC, LANES), lambda k: (0, 0, k, 0, 0))
    out = pl.BlockSpec((2, 2 * KEEP, 2 * KEEP), lambda k: (k + base, 0, 0))
    extra = [] if before is None else [before]
    count = len(values)
    return pl.pallas_call(
        functools.partial(second_kernel, count, [s[0] for s in sides], [len(s) - 1 for s in sides], base),
        grid=(pairs,),
        in_specs=[pl.BlockSpec(memory_space=pltpu.SMEM), pl.BlockSpec(table.shape, lambda k: (0,) * 3)]
        + [block] * count
        + [out] * len(extra),
        out_specs=out,
        out_shape=jax.ShapeDtypeStruct((2 * PAIRS, 2 * KEEP, 2 * KEEP), jnp.float32),
        input_output_aliases={2 + count: 0} if extra else {},
        compiler_params=params(),
        cost_estimate=pl.CostEstimate(
            flops=pairs * len(sides) * 320 * 256 * 640 * 6, bytes_accessed=3_000_000 * pairs, transcendentals=0
        ),
    )(place, table, *values, *extra)


def ring(value, flip_high, flip_low):
    moves = [(2 * h + l, 2 * (h ^ flip_high) + (l ^ flip_low)) for h in range(2) for l in range(2)]
    return lax.ppermute(value, ("xh", "xl"), moves)


def spread(value):
    return lax.all_to_all(value, ("z", "y"), split_axis=0, concat_axis=0, tiled=True)


def transform(velocity_u, velocity_v, scalar_theta):
    high, core, low = lax.axis_index("xh"), lax.axis_index("core"), lax.axis_index("xl")
    owns_mean = (low == 1) & (lax.axis_index("z") == 0) & (lax.axis_index("y") == 0)
    place = jnp.stack([core, high, owns_mean.astype(jnp.int32), low]).astype(jnp.int32)

    rows = jnp.asarray(first_table())
    columns = jnp.asarray(depth_table())
    fields = (velocity_u, velocity_v, scalar_theta)

    def depth(unit, keeps):
        return depth_stage(place, *fields, columns, int(unit[0]), int(unit[1]), keeps)

    def swap(send):
        return lax.ppermute(send, "core", [(0, 1), (1, 0)])

    def first(own, recv, blocks, splits):
        return first_stage(place, own, recv, rows, blocks, splits)

    def near_ring(values):
        return [ring(value, 1, 0) for value in values]

    def far_ring(unit, values):
        return [ring(value, int(unit[1]), 1) for value in values]

    def gather(a, b):
        return spread(jnp.add(a, b))

    def second(chunk, sides, base, result):
        return second_stage(place, jnp.asarray(second_table(chunk)), sides, base, result)

    (send,) = depth("01", (0,))
    recv = swap(send)
    (own,) = depth("01", (1,))
    near = near_ring(first(own, recv, (0,), ((PAIRS,),)))
    far, far_early = first(own, recv, (1,), (EARLY,))
    far = far_ring("01", [far])

    send, own = depth("00", (0, 1))
    kept, across, across_early = first(own, swap(send), (0, 1), ((PAIRS,), EARLY))
    across = far_ring("00", [across])

    early = spread(jnp.stack([across_early, far_early], axis=1))
    across_early = ring(early[:, 0], 0, 1)
    far_early = ring(early[:, 1], 1, 1)

    send, own = depth("11", (0, 1))
    near_last, far_last = first(own, swap(send), (0, 1), ((PAIRS,), (PAIRS,)))
    near_last = near_ring([near_last])
    far_last = far_ring("11", [far_last])

    send, own = depth("10", (0, 1))
    kept_last, across_last = first(own, swap(send), (0, 1), ((PAIRS,), (PAIRS,)))
    across_last = far_ring("10", [across_last])

    mine = gather(kept, near[0])
    other = gather(across[0], far[0])
    mine_last = gather(kept_last, near_last[0])
    other_last = gather(across_last[0], far_last[0])

    result = second(0, [(0, mine)], 0, None)
    result = second(0, [(1, other)], 0, result)
    result = second(1, [(0, mine_last)], 0, result)
    result = second(0, [(1, across_early, far_early)], EARLY[0], result)
    result = second(1, [(1, other_last)], 0, result)
    return result[None]


def solution(mesh):
    fine = Mesh(mesh.devices.reshape(2, 2, 2, 4, 4), ("xh", "core", "xl", "z", "y"))
    spec = P(("xh", "core"), ("xl", "z", "y"), None)
    out_specs = P(("xh", "core"), ("xl", "z", "y"), None, None)
    return jax.shard_map(transform, mesh=fine, in_specs=(spec,) * 3, out_specs=out_specs, check_vma=False)
```

```python
import functools

import jax
import jax.numpy as jnp
import ml_dtypes
import numpy as np
from jax import lax
from jax.experimental import pallas as pl
from jax.experimental.pallas import tpu as pltpu
from jax.sharding import Mesh
from jax.sharding import PartitionSpec as P


N = 512
KEEP = 160
LANES = 128
XB = 128
XSTEP = 32
YC = 8
DESTS = 16
PAIRS = 5
EARLY = (3, 2)
VMEM_LIMIT = 24 * 1024 * 1024
DEPTH_LIMIT = 50 * 1024 * 1024


def split_table(table):
    high = table.astype(ml_dtypes.bfloat16)
    low = (table - high.astype(np.float64)).astype(ml_dtypes.bfloat16)
    return np.stack([high, low])


def angles(places, waves):
    return (places * waves % N) * (2.0 * np.pi / N)


def depth_table():
    angle = angles(np.arange(N)[:, None], np.arange(KEEP)[None, :])
    re, im = np.cos(angle), -np.sin(angle)
    zeros = np.zeros((N, 64))
    table = np.concatenate([re[:, :128], im[:, :128], re[:, 128:], im[:, 128:], zeros], axis=1)
    return split_table(table / np.sqrt(N))


def first_table():
    half, e, pair, dest = np.meshgrid(np.arange(2), np.arange(2), np.arange(5), np.arange(16), indexing="ij")
    waves = (half * 160 + dest * 10 + 2 * pair + e - KEEP).reshape(2, KEEP)
    angle = angles(np.arange(XB)[None, None, :], waves[:, :, None])
    table = np.stack([np.cos(angle), np.sin(angle)], axis=1)
    return split_table(table / np.sqrt(N))


def second_table(chunk):
    source, y = np.meshgrid(np.arange(16), np.arange(YC), indexing="ij")
    places = (source * 16 + chunk * YC + y).reshape(-1)
    waves = np.arange(2 * KEEP) - KEEP
    angle = angles(places[None, :], waves[:, None])
    table = np.concatenate([np.cos(angle), np.sin(angle)], axis=1)
    return split_table(table / np.sqrt(N))


def halves(value):
    high = value.astype(jnp.bfloat16)
    return high, (value - high.astype(jnp.float32)).astype(jnp.bfloat16)


def dot(a, b):
    return jnp.dot(a, b, preferred_element_type=jnp.float32)


def turn_tail(tail):
    lane = lax.broadcasted_iota(jnp.int32, tail.shape, 1)
    return jnp.where(lane % 64 < 32, pltpu.roll(tail, 96, 1), -pltpu.roll(tail, 32, 1))


def params(limit=VMEM_LIMIT):
    return pltpu.CompilerParams(vmem_limit_bytes=limit)


def depth_kernel(chunk, group, keeps, place_ref, table_ref, *refs):
    count = len(keeps)
    fields, outs = refs[:3], refs[3 : 3 + count]
    held, made, in_sems, out_sems = refs[3 + count :]
    first = place_ref[0] == 0
    squares = place_ref[1] == group
    rows = YC * XSTEP

    def load(f, i):
        source = fields[f].at[pl.ds(i * XSTEP, XSTEP), pl.ds(chunk * YC, YC)]
        return pltpu.make_async_copy(source, held.at[f, i], in_sems.at[f, i])

    def save(k, i):
        target = outs[k].at[:, pl.ds(i * XSTEP, XSTEP)]
        return pltpu.make_async_copy(made.at[k, i], target, out_sems.at[k, i])

    for i in range(XB // XSTEP):
        for f in range(3):
            load(f, i).start()

    def step(i, carry):
        for f in range(3):
            load(f, i).wait()
        u, v, t = held[0, i], held[1, i], held[2, i]
        highs, lows = [], []
        for keep in keeps:
            swap = first if keep == 0 else ~first
            a = jnp.where(squares & swap, v, u)
            product = a * jnp.where(squares, a, jnp.where(swap, t, v))
            high, low = halves(jnp.swapaxes(product, 0, 1).reshape(rows, N))
            highs.append(high)
            lows.append(low)
        high, low = jnp.concatenate(highs, axis=0), jnp.concatenate(lows, axis=0)
        table = jnp.concatenate([table_ref[0], table_ref[0], table_ref[1]], axis=0)
        out = dot(jnp.concatenate([high, low, high], axis=1), table)
        for k in range(count):
            made[k, i] = out[k * rows : (k + 1) * rows].reshape(YC, XSTEP, 384)
            save(k, i).start()
        return carry

    lax.fori_loop(0, XB // XSTEP, step, 0)
    for i in range(XB // XSTEP):
        for k in range(count):
            save(k, i).wait()


def depth_stage(place, u, v, t, table, chunk, group, keeps):
    steps, count = XB // XSTEP, len(keeps)
    shape = jax.ShapeDtypeStruct((YC, XB, 384), jnp.float32)
    far = pl.BlockSpec(memory_space=pltpu.HBM)
    return pl.pallas_call(
        functools.partial(depth_kernel, chunk, group, keeps),
        in_specs=[pl.BlockSpec(memory_space=pltpu.SMEM), pl.BlockSpec(memory_space=pltpu.VMEM), far, far, far],
        out_specs=[far] * count,
        out_shape=[shape] * count,
        scratch_shapes=[
            pltpu.VMEM((3, steps, XSTEP, YC, N), jnp.float32),
            pltpu.VMEM((count, steps, YC, XSTEP, 384), jnp.float32),
            pltpu.SemaphoreType.DMA((3, steps)),
            pltpu.SemaphoreType.DMA((count, steps)),
        ],
        compiler_params=params(DEPTH_LIMIT),
        cost_estimate=pl.CostEstimate(flops=count * XB * YC * N * 384 * 6, bytes_accessed=9_000_000, transcendentals=0),
    )(place, table, u, v, t)


def first_kernel(blocks, splits, place_ref, own_ref, recv_ref, table_ref, *refs):
    core, high_half, low_half = place_ref[0], place_ref[1], place_ref[3]
    step = pl.program_id(0)
    sides = []
    for y in range(2):
        values = jnp.concatenate([own_ref[y], recv_ref[y]], axis=0)
        re, im, tail = values[:, :128], values[:, 128:256], values[:, 256:]
        sides.append(jnp.concatenate([values, jnp.concatenate([im, -re, turn_tail(tail)], axis=1)], axis=0))
    high, low = halves(jnp.concatenate(sides, axis=1))
    data = jnp.concatenate([high, low, high], axis=0)

    row = lax.broadcasted_iota(jnp.int32, (KEEP, 1), 0)
    e = row // 80
    q = (row // 16 + row + e) & 1
    turns = [jnp.where(flip == 1, -1.0, 1.0).astype(jnp.bfloat16) for flip in (q ^ e, q)]

    def rows_of(half):
        parts = []
        for part in range(2):
            plain = [table_ref[part, half, cs] for cs in range(2)]
            moved = [jnp.concatenate([plain[cs][:80], plain[1 - cs][80:]], axis=0) * turns[cs] for cs in range(2)]
            parts.append([jnp.where(core == j, plain[cs], moved[cs]) for cs in range(2) for j in range(2)])
        return jnp.concatenate(parts[0] + parts[0] + parts[1], axis=1)

    out = dot(jnp.concatenate([rows_of(low_half ^ b) for b in blocks], axis=0), data)
    sign = jnp.where(high_half == 1, -1.0, 1.0)
    index = 0
    for b in range(len(blocks)):
        base = 0
        for pairs in splits[b]:
            ref = refs[index]
            index += 1
            stride = 5 * pairs * YC
            for y in range(2):
                for p in range(pairs):
                    row = b * 160 + (base + p) * DESTS
                    even = out[row : row + DESTS, 384 * y : 384 * (y + 1)]
                    odd = out[row + 80 : row + 80 + DESTS, 384 * y : 384 * (y + 1)] * sign
                    tiles = [even[:, :128], even[:, 128:256], odd[:, :128], odd[:, 128:256]]
                    tiles.append(even[:, 256:] + pltpu.roll(odd[:, 256:], 64, 1))
                    for i, tile in enumerate(tiles):
                        start = (i * pairs + p) * YC + 2 * step + y
                        ref[pl.ds(start, DESTS, stride=stride), :] = tile
            base += pairs


def first_stage(place, own, recv, table, blocks, splits):
    block = pl.BlockSpec((2, XB, 384), lambda i: (i, 0, 0))
    sizes = [pairs for split in splits for pairs in split]
    outs = [(DESTS * 5 * pairs * YC, LANES) for pairs in sizes]
    results = pl.pallas_call(
        functools.partial(first_kernel, blocks, splits),
        grid=(YC // 2,),
        in_specs=[
            pl.BlockSpec(memory_space=pltpu.SMEM),
            block,
            block,
            pl.BlockSpec(table.shape, lambda i: (0,) * 5),
        ],
        out_specs=[pl.BlockSpec(shape, lambda i: (0, 0)) for shape in outs],
        out_shape=[jax.ShapeDtypeStruct(shape, jnp.float32) for shape in outs],
        compiler_params=params(DEPTH_LIMIT),
        cost_estimate=pl.CostEstimate(flops=YC * len(blocks) * 160 * 512 * 384 * 6, bytes_accessed=7_000_000, transcendentals=0),
    )(place, own, recv, table)
    return [r.reshape(DESTS, 5, pairs, YC, LANES) for r, pairs in zip(results, sizes)]


def second_kernel(fresh, parts, base, pairs, adds, place_ref, table_ref, *refs):
    count = sum(parts)
    sides, past, out_ref = refs[:count], refs[count], refs[count + adds]
    held, total, in_sems, past_sems, out_sems = refs[count + adds + 1 :]

    def load(s, p):
        return pltpu.make_async_copy(sides[s].at[:, :, p], held.at[s, p], in_sems.at[s, p])

    def recall(p):
        return pltpu.make_async_copy(past.at[pl.ds(2 * (p + base), 2)], total.at[p], past_sems.at[p])

    def save(p):
        return pltpu.make_async_copy(total.at[p], out_ref.at[pl.ds(2 * (p + base), 2)], out_sems.at[p])

    for p in range(pairs):
        for s in range(count):
            load(s, p).start()
        if adds:
            recall(p).start()

    def step(p, carry):
        left, right = [], []
        at = 0
        for s in range(count):
            load(s, p).wait()
        for side in range(len(fresh)):
            group = range(at, at + parts[side])
            at += parts[side]
            t = [sum(held[s, p, :, i].reshape(DESTS * YC, LANES) for s in group) for i in range(5)]
            values = jnp.concatenate(t, axis=1)
            turned = jnp.concatenate([t[1], -t[0], t[3], -t[2], turn_tail(t[4])], axis=1)
            high, low = halves(jnp.concatenate([values, turned], axis=0))
            odd = lax.broadcasted_iota(jnp.int32, (2 * KEEP, 1), 0) % 2 == 1
            flip = odd & ((place_ref[3] ^ fresh[side]) == 1)
            sign = jnp.where(flip, -1.0, 1.0).astype(jnp.bfloat16)
            left += [table_ref[0] * sign, table_ref[0] * sign, table_ref[1] * sign]
            right += [high, low, high]
        out = dot(jnp.concatenate(left, axis=1), jnp.concatenate(right, axis=0))
        tail = out[:, 512:]
        lane = lax.broadcasted_iota(jnp.int32, tail.shape, 1)
        if adds:
            recall(p).wait()
        for e in range(2):
            re, im = out[:, 256 * e : 256 * e + 128], out[:, 256 * e + 128 : 256 * e + 256]
            moved = pltpu.roll(im, 32, 1)
            ends = tail if e == 0 else pltpu.roll(tail, 64, 1)
            pieces = [re, jnp.where(lane < 32, ends, moved), jnp.where(lane < 32, moved, ends)[:, :64]]
            for i, piece in enumerate(pieces):
                span = slice(128 * i, min(128 * (i + 1), 320))
                total[p, e, :, span] = piece + total[p, e, :, span] if adds else piece

        @pl.when((place_ref[2] == 1) & (p + base == 0))
        def _():
            row = total[0, 0, KEEP : KEEP + 1, 0:128]
            first = lax.broadcasted_iota(jnp.int32, row.shape, 1) == 0
            total[0, 0, KEEP : KEEP + 1, 0:128] = jnp.where(first, 0.0, row)

        save(p).start()
        return carry

    lax.fori_loop(0, pairs, step, 0)
    for p in range(pairs):
        save(p).wait()


def second_stage(place, table, sides, base, before):
    values = [value for side in sides for value in side[1:]]
    pairs = values[0].shape[2]
    extra = [] if before is None else [before]
    count = len(values)
    far = pl.BlockSpec(memory_space=pltpu.HBM)
    parts = [len(s) - 1 for s in sides]
    return pl.pallas_call(
        functools.partial(second_kernel, [s[0] for s in sides], parts, base, pairs, len(extra)),
        in_specs=[pl.BlockSpec(memory_space=pltpu.SMEM), pl.BlockSpec(memory_space=pltpu.VMEM)]
        + [far] * (count + len(extra)),
        out_specs=far,
        out_shape=jax.ShapeDtypeStruct((2 * PAIRS, 2 * KEEP, 2 * KEEP), jnp.float32),
        scratch_shapes=[
            pltpu.VMEM((count, pairs, DESTS, 5, YC, LANES), jnp.float32),
            pltpu.VMEM((pairs, 2, 2 * KEEP, 2 * KEEP), jnp.float32),
            pltpu.SemaphoreType.DMA((count, pairs)),
            pltpu.SemaphoreType.DMA((pairs,)),
            pltpu.SemaphoreType.DMA((pairs,)),
        ],
        input_output_aliases={2 + count: 0} if extra else {},
        compiler_params=params(),
        cost_estimate=pl.CostEstimate(
            flops=pairs * len(sides) * 320 * 256 * 640 * 6, bytes_accessed=3_000_000 * pairs, transcendentals=0
        ),
    )(place, table, *values, *extra)


def ring(value, flip_high, flip_low):
    moves = [(2 * h + l, 2 * (h ^ flip_high) + (l ^ flip_low)) for h in range(2) for l in range(2)]
    return lax.ppermute(value, ("xh", "xl"), moves)


def spread(value):
    return lax.all_to_all(value, ("z", "y"), split_axis=0, concat_axis=0, tiled=True)


def transform(velocity_u, velocity_v, scalar_theta):
    high, core, low = lax.axis_index("xh"), lax.axis_index("core"), lax.axis_index("xl")
    owns_mean = (low == 1) & (lax.axis_index("z") == 0) & (lax.axis_index("y") == 0)
    place = jnp.stack([core, high, owns_mean.astype(jnp.int32), low]).astype(jnp.int32)

    rows = jnp.asarray(first_table())
    columns = jnp.asarray(depth_table())
    fields = (velocity_u, velocity_v, scalar_theta)

    def depth(unit, keeps):
        return depth_stage(place, *fields, columns, int(unit[0]), int(unit[1]), keeps)

    def swap(send):
        return lax.ppermute(send, "core", [(0, 1), (1, 0)])

    def first(own, recv, blocks, splits):
        return first_stage(place, own, recv, rows, blocks, splits)

    def near_ring(values):
        return [ring(value, 1, 0) for value in values]

    def far_ring(unit, values):
        return [ring(value, int(unit[1]), 1) for value in values]

    def gather(a, b):
        return spread(jnp.add(a, b))

    def second(chunk, sides, base, result):
        return second_stage(place, jnp.asarray(second_table(chunk)), sides, base, result)

    (send,) = depth("01", (0,))
    recv = swap(send)
    (own,) = depth("01", (1,))
    near = near_ring(first(own, recv, (0,), ((PAIRS,),)))
    far, far_early = first(own, recv, (1,), (EARLY,))
    far = far_ring("01", [far])

    send, own = depth("00", (0, 1))
    kept, across, across_early = first(own, swap(send), (0, 1), ((PAIRS,), EARLY))
    across = far_ring("00", [across])

    early = spread(jnp.stack([across_early, far_early], axis=1))
    across_early = ring(early[:, 0], 0, 1)
    far_early = ring(early[:, 1], 1, 1)

    send, own = depth("11", (0, 1))
    near_last, far_last = first(own, swap(send), (0, 1), ((PAIRS,), (PAIRS,)))
    near_last = near_ring([near_last])
    far_last = far_ring("11", [far_last])

    send, own = depth("10", (0, 1))
    kept_last, across_last = first(own, swap(send), (0, 1), ((PAIRS,), (PAIRS,)))
    across_last = far_ring("10", [across_last])

    mine = gather(kept, near[0])
    other = gather(across[0], far[0])
    mine_last = gather(kept_last, near_last[0])
    other_last = gather(across_last[0], far_last[0])

    result = second(0, [(0, mine)], 0, None)
    result = second(0, [(1, other)], 0, result)
    result = second(1, [(0, mine_last)], 0, result)
    result = second(0, [(1, across_early, far_early)], EARLY[0], result)
    result = second(1, [(1, other_last)], 0, result)
    return result[None]


def solution(mesh):
    fine = Mesh(mesh.devices.reshape(2, 2, 2, 4, 4), ("xh", "core", "xl", "z", "y"))
    spec = P(("xh", "core"), ("xl", "z", "y"), None)
    out_specs = P(("xh", "core"), ("xl", "z", "y"), None, None)
    return jax.shard_map(transform, mesh=fine, in_specs=(spec,) * 3, out_specs=out_specs, check_vma=False)
```

```python
import functools

import jax
import jax.numpy as jnp
import ml_dtypes
import numpy as np
from jax import lax
from jax.experimental import pallas as pl
from jax.experimental.pallas import tpu as pltpu
from jax.sharding import Mesh
from jax.sharding import PartitionSpec as P


N = 512
KEEP = 160
LANES = 128
XB = 128
YC = 8
DESTS = 16
PAIRS = 5
EARLY = (3, 2)
VMEM_LIMIT = 24 * 1024 * 1024
DEPTH_LIMIT = 48 * 1024 * 1024


def split_table(table):
    high = table.astype(ml_dtypes.bfloat16)
    low = (table - high.astype(np.float64)).astype(ml_dtypes.bfloat16)
    return np.stack([high, low])


def angles(places, waves):
    return (places * waves % N) * (2.0 * np.pi / N)


def depth_table():
    angle = angles(np.arange(N)[:, None], np.arange(KEEP)[None, :])
    re, im = np.cos(angle), -np.sin(angle)
    zeros = np.zeros((N, 64))
    table = np.concatenate([re[:, :128], im[:, :128], re[:, 128:], im[:, 128:], zeros], axis=1)
    return split_table(table / np.sqrt(N))


def first_table():
    half, e, pair, dest = np.meshgrid(np.arange(2), np.arange(2), np.arange(5), np.arange(16), indexing="ij")
    waves = (half * 160 + dest * 10 + 2 * pair + e - KEEP).reshape(2, KEEP)
    angle = angles(np.arange(XB)[None, None, :], waves[:, :, None])
    table = np.stack([np.cos(angle), np.sin(angle)], axis=1)
    return split_table(table / np.sqrt(N))


def second_table(chunk):
    source, y = np.meshgrid(np.arange(16), np.arange(YC), indexing="ij")
    places = (source * 16 + chunk * YC + y).reshape(-1)
    waves = np.arange(2 * KEEP) - KEEP
    angle = angles(places[None, :], waves[:, None])
    table = np.concatenate([np.cos(angle), np.sin(angle)], axis=1)
    return split_table(table / np.sqrt(N))


def halves(value):
    high = value.astype(jnp.bfloat16)
    return high, (value - high.astype(jnp.float32)).astype(jnp.bfloat16)


def dot(a, b):
    return jnp.dot(a, b, preferred_element_type=jnp.float32)


def turn_tail(tail):
    lane = lax.broadcasted_iota(jnp.int32, tail.shape, 1)
    return jnp.where(lane % 64 < 32, pltpu.roll(tail, 96, 1), -pltpu.roll(tail, 32, 1))


def params(limit=VMEM_LIMIT):
    return pltpu.CompilerParams(vmem_limit_bytes=limit)


def depth_kernel(group, keeps, place_ref, u_ref, v_ref, t_ref, table_ref, *out_refs):
    first = place_ref[0] == 0
    squares = place_ref[1] == group
    u, v, t = u_ref[...], v_ref[...], t_ref[...]
    rows = YC * u.shape[0]
    highs, lows = [], []
    for keep in keeps:
        swap = first if keep == 0 else ~first
        a = jnp.where(squares & swap, v, u)
        product = a * jnp.where(squares, a, jnp.where(swap, t, v))
        high, low = halves(jnp.swapaxes(product, 0, 1).reshape(rows, N))
        highs.append(high)
        lows.append(low)
    high, low = jnp.concatenate(highs, axis=0), jnp.concatenate(lows, axis=0)
    table = jnp.concatenate([table_ref[0], table_ref[0], table_ref[1]], axis=0)
    out = dot(jnp.concatenate([high, low, high], axis=1), table)
    for i, ref in enumerate(out_refs):
        ref[...] = out[i * rows : (i + 1) * rows].reshape(YC, rows // YC, 384)


def depth_stage(place, u, v, t, table, chunk, group, keeps):
    xb = 32
    block = pl.BlockSpec((xb, YC, N), lambda i: (i, chunk, 0))
    out = pl.BlockSpec((YC, xb, 384), lambda i: (0, i, 0))
    shape = jax.ShapeDtypeStruct((YC, XB, 384), jnp.float32)
    return pl.pallas_call(
        functools.partial(depth_kernel, group, keeps),
        grid=(XB // xb,),
        in_specs=[
            pl.BlockSpec(memory_space=pltpu.SMEM),
            block,
            block,
            block,
            pl.BlockSpec((2, N, 384), lambda i: (0, 0, 0)),
        ],
        out_specs=[out] * len(keeps),
        out_shape=[shape] * len(keeps),
        compiler_params=params(DEPTH_LIMIT),
        cost_estimate=pl.CostEstimate(
            flops=len(keeps) * XB * YC * N * 384 * 6, bytes_accessed=9_000_000, transcendentals=0
        ),
    )(place, u, v, t, table)


def first_kernel(blocks, splits, place_ref, own_ref, recv_ref, table_ref, *refs):
    core, high_half, low_half = place_ref[0], place_ref[1], place_ref[3]
    step = pl.program_id(0)
    sides = []
    for y in range(2):
        values = jnp.concatenate([own_ref[y], recv_ref[y]], axis=0)
        re, im, tail = values[:, :128], values[:, 128:256], values[:, 256:]
        sides.append(jnp.concatenate([values, jnp.concatenate([im, -re, turn_tail(tail)], axis=1)], axis=0))
    high, low = halves(jnp.concatenate(sides, axis=1))
    data = jnp.concatenate([high, low, high], axis=0)

    row = lax.broadcasted_iota(jnp.int32, (KEEP, 1), 0)
    e = row // 80
    q = (row // 16 + row + e) & 1
    turns = [jnp.where(flip == 1, -1.0, 1.0).astype(jnp.bfloat16) for flip in (q ^ e, q)]

    def rows_of(half):
        parts = []
        for part in range(2):
            plain = [table_ref[part, half, cs] for cs in range(2)]
            moved = [jnp.concatenate([plain[cs][:80], plain[1 - cs][80:]], axis=0) * turns[cs] for cs in range(2)]
            parts.append([jnp.where(core == j, plain[cs], moved[cs]) for cs in range(2) for j in range(2)])
        return jnp.concatenate(parts[0] + parts[0] + parts[1], axis=1)

    out = dot(jnp.concatenate([rows_of(low_half ^ b) for b in blocks], axis=0), data)
    sign = jnp.where(high_half == 1, -1.0, 1.0)
    index = 0
    for b in range(len(blocks)):
        base = 0
        for pairs in splits[b]:
            ref = refs[index]
            index += 1
            stride = 5 * pairs * YC
            for y in range(2):
                for p in range(pairs):
                    row = b * 160 + (base + p) * DESTS
                    even = out[row : row + DESTS, 384 * y : 384 * (y + 1)]
                    odd = out[row + 80 : row + 80 + DESTS, 384 * y : 384 * (y + 1)] * sign
                    tiles = [even[:, :128], even[:, 128:256], odd[:, :128], odd[:, 128:256]]
                    tiles.append(even[:, 256:] + pltpu.roll(odd[:, 256:], 64, 1))
                    for i, tile in enumerate(tiles):
                        start = (i * pairs + p) * YC + 2 * step + y
                        ref[pl.ds(start, DESTS, stride=stride), :] = tile
            base += pairs


def first_stage(place, own, recv, table, blocks, splits):
    block = pl.BlockSpec((2, XB, 384), lambda i: (i, 0, 0))
    sizes = [pairs for split in splits for pairs in split]
    outs = [(DESTS * 5 * pairs * YC, LANES) for pairs in sizes]
    results = pl.pallas_call(
        functools.partial(first_kernel, blocks, splits),
        grid=(YC // 2,),
        in_specs=[
            pl.BlockSpec(memory_space=pltpu.SMEM),
            block,
            block,
            pl.BlockSpec(table.shape, lambda i: (0,) * 5),
        ],
        out_specs=[pl.BlockSpec(shape, lambda i: (0, 0)) for shape in outs],
        out_shape=[jax.ShapeDtypeStruct(shape, jnp.float32) for shape in outs],
        compiler_params=params(DEPTH_LIMIT),
        cost_estimate=pl.CostEstimate(flops=YC * len(blocks) * 160 * 512 * 384 * 6, bytes_accessed=7_000_000, transcendentals=0),
    )(place, own, recv, table)
    return [r.reshape(DESTS, 5, pairs, YC, LANES) for r, pairs in zip(results, sizes)]


def second_kernel(fresh, parts, base, pairs, adds, place_ref, table_ref, *refs):
    count = sum(parts)
    sides, past, out_ref = refs[:count], refs[count], refs[count + adds]
    held, total, in_sems, past_sems, out_sems = refs[count + adds + 1 :]

    def load(s, p):
        return pltpu.make_async_copy(sides[s].at[:, :, p], held.at[s, p], in_sems.at[s, p])

    def recall(p):
        return pltpu.make_async_copy(past.at[pl.ds(2 * (p + base), 2)], total.at[p], past_sems.at[p])

    def save(p):
        return pltpu.make_async_copy(total.at[p], out_ref.at[pl.ds(2 * (p + base), 2)], out_sems.at[p])

    def fetch(p):
        for s in range(count):
            load(s, p).start()
        if adds:
            recall(p).start()

    fetch(0)
    fetch(1)

    def step(p, carry):
        left, right = [], []
        at = 0

        @pl.when(p + 2 < pairs)
        def _():
            fetch(p + 2)

        for s in range(count):
            load(s, p).wait()
        for side in range(len(fresh)):
            group = range(at, at + parts[side])
            at += parts[side]
            t = [sum(held[s, p, :, i].reshape(DESTS * YC, LANES) for s in group) for i in range(5)]
            values = jnp.concatenate(t, axis=1)
            turned = jnp.concatenate([t[1], -t[0], t[3], -t[2], turn_tail(t[4])], axis=1)
            high, low = halves(jnp.concatenate([values, turned], axis=0))
            odd = lax.broadcasted_iota(jnp.int32, (2 * KEEP, 1), 0) % 2 == 1
            flip = odd & ((place_ref[3] ^ fresh[side]) == 1)
            sign = jnp.where(flip, -1.0, 1.0).astype(jnp.bfloat16)
            left += [table_ref[0] * sign, table_ref[0] * sign, table_ref[1] * sign]
            right += [high, low, high]
        out = dot(jnp.concatenate(left, axis=1), jnp.concatenate(right, axis=0))
        tail = out[:, 512:]
        lane = lax.broadcasted_iota(jnp.int32, tail.shape, 1)
        if adds:
            recall(p).wait()
        for e in range(2):
            re, im = out[:, 256 * e : 256 * e + 128], out[:, 256 * e + 128 : 256 * e + 256]
            moved = pltpu.roll(im, 32, 1)
            ends = tail if e == 0 else pltpu.roll(tail, 64, 1)
            pieces = [re, jnp.where(lane < 32, ends, moved), jnp.where(lane < 32, moved, ends)[:, :64]]
            for i, piece in enumerate(pieces):
                span = slice(128 * i, min(128 * (i + 1), 320))
                total[p, e, :, span] = piece + total[p, e, :, span] if adds else piece

        @pl.when((place_ref[2] == 1) & (p + base == 0))
        def _():
            row = total[0, 0, KEEP : KEEP + 1, 0:128]
            first = lax.broadcasted_iota(jnp.int32, row.shape, 1) == 0
            total[0, 0, KEEP : KEEP + 1, 0:128] = jnp.where(first, 0.0, row)

        save(p).start()
        return carry

    lax.fori_loop(0, pairs, step, 0)
    for p in range(pairs):
        save(p).wait()


def second_stage(place, table, sides, base, before):
    values = [value for side in sides for value in side[1:]]
    pairs = values[0].shape[2]
    extra = [] if before is None else [before]
    count = len(values)
    far = pl.BlockSpec(memory_space=pltpu.HBM)
    parts = [len(s) - 1 for s in sides]
    return pl.pallas_call(
        functools.partial(second_kernel, [s[0] for s in sides], parts, base, pairs, len(extra)),
        in_specs=[pl.BlockSpec(memory_space=pltpu.SMEM), pl.BlockSpec(memory_space=pltpu.VMEM)]
        + [far] * (count + len(extra)),
        out_specs=far,
        out_shape=jax.ShapeDtypeStruct((2 * PAIRS, 2 * KEEP, 2 * KEEP), jnp.float32),
        scratch_shapes=[
            pltpu.VMEM((count, pairs, DESTS, 5, YC, LANES), jnp.float32),
            pltpu.VMEM((pairs, 2, 2 * KEEP, 2 * KEEP), jnp.float32),
            pltpu.SemaphoreType.DMA((count, pairs)),
            pltpu.SemaphoreType.DMA((pairs,)),
            pltpu.SemaphoreType.DMA((pairs,)),
        ],
        input_output_aliases={2 + count: 0} if extra else {},
        compiler_params=params(),
        cost_estimate=pl.CostEstimate(
            flops=pairs * len(sides) * 320 * 256 * 640 * 6, bytes_accessed=3_000_000 * pairs, transcendentals=0
        ),
    )(place, table, *values, *extra)


def ring(value, flip_high, flip_low):
    moves = [(2 * h + l, 2 * (h ^ flip_high) + (l ^ flip_low)) for h in range(2) for l in range(2)]
    return lax.ppermute(value, ("xh", "xl"), moves)


def spread(value):
    return lax.all_to_all(value, ("z", "y"), split_axis=0, concat_axis=0, tiled=True)


def transform(velocity_u, velocity_v, scalar_theta):
    high, core, low = lax.axis_index("xh"), lax.axis_index("core"), lax.axis_index("xl")
    owns_mean = (low == 1) & (lax.axis_index("z") == 0) & (lax.axis_index("y") == 0)
    place = jnp.stack([core, high, owns_mean.astype(jnp.int32), low]).astype(jnp.int32)

    rows = jnp.asarray(first_table())
    columns = jnp.asarray(depth_table())
    fields = (velocity_u, velocity_v, scalar_theta)

    def depth(unit, keeps):
        return depth_stage(place, *fields, columns, int(unit[0]), int(unit[1]), keeps)

    def swap(send):
        return lax.ppermute(send, "core", [(0, 1), (1, 0)])

    def first(own, recv, blocks, splits):
        return first_stage(place, own, recv, rows, blocks, splits)

    def near_ring(values):
        return [ring(value, 1, 0) for value in values]

    def far_ring(unit, values):
        return [ring(value, int(unit[1]), 1) for value in values]

    def gather(a, b):
        return spread(jnp.add(a, b))

    def second(chunk, sides, base, result):
        return second_stage(place, jnp.asarray(second_table(chunk)), sides, base, result)

    (send,) = depth("01", (0,))
    recv = swap(send)
    (own,) = depth("01", (1,))
    near = near_ring(first(own, recv, (0,), ((PAIRS,),)))
    far, far_early = first(own, recv, (1,), (EARLY,))
    far = far_ring("01", [far])

    send, own = depth("00", (0, 1))
    kept, across, across_early = first(own, swap(send), (0, 1), ((PAIRS,), EARLY))
    across = far_ring("00", [across])

    early = spread(jnp.stack([across_early, far_early], axis=1))
    across_early = ring(early[:, 0], 0, 1)
    far_early = ring(early[:, 1], 1, 1)

    send, own = depth("11", (0, 1))
    near_last, far_last = first(own, swap(send), (0, 1), ((PAIRS,), (PAIRS,)))
    near_last = near_ring([near_last])
    far_last = far_ring("11", [far_last])

    send, own = depth("10", (0, 1))
    kept_last, across_last = first(own, swap(send), (0, 1), ((PAIRS,), (PAIRS,)))
    across_last = far_ring("10", [across_last])

    mine = gather(kept, near[0])
    other = gather(across[0], far[0])
    mine_last = gather(kept_last, near_last[0])
    other_last = gather(across_last[0], far_last[0])

    result = second(0, [(0, mine)], 0, None)
    result = second(0, [(1, other)], 0, result)
    result = second(1, [(0, mine_last)], 0, result)
    result = second(0, [(1, across_early, far_early)], EARLY[0], result)
    result = second(1, [(1, other_last)], 0, result)
    return result[None]


def solution(mesh):
    fine = Mesh(mesh.devices.reshape(2, 2, 2, 4, 4), ("xh", "core", "xl", "z", "y"))
    spec = P(("xh", "core"), ("xl", "z", "y"), None)
    out_specs = P(("xh", "core"), ("xl", "z", "y"), None, None)
    return jax.shard_map(transform, mesh=fine, in_specs=(spec,) * 3, out_specs=out_specs, check_vma=False)
```
